32 devices in a mesh: gx: 4 (over z), gy: 8 (over y, x, core).
Axes of the slice: x: 2, y: 2, z: 4, core: 2. Of those that a mesh axis runs over, the one named last changes fastest.
Arguments:
- x_gen: bfloat16 [8, 512, 3072], P('gy', 'gx'), may hold values from -6 to 6
- fresh_noise: bfloat16 [8, 512, 3072], P('gy', 'gx'), may hold values from -6 to 6
- steps_t: int32 [8], P('gy'), may hold values from 0 to 999
- real_mod: float32 [8, 2, 3072], P('gy'), may hold values from -2.5 to 2.5
- real_w_up: bfloat16 [3072, 6144], P(None, 'gx'), may hold values from -0.109375 to 0.109375
- real_b_up: float32 [6144], P('gx'), may hold values from -3 to 3
- real_w_down: bfloat16 [6144, 3072], P('gx'), may hold values from -0.078125 to 0.078125
- fake_mod: float32 [8, 2, 3072], P('gy'), may hold values from -2.5 to 2.5
- fake_w_up: bfloat16 [3072, 6144], P('gy', 'gx'), may hold values from -0.109375 to 0.109375
- fake_b_up: float32 [6144], P('gx'), may hold values from -3 to 3
- fake_w_down: bfloat16 [6144, 3072], P('gx', 'gy'), may hold values from -0.078125 to 0.078125
Outputs:
- dmd_grad: float32 [8, 512, 3072], P('gy', 'gx')
- fake_grad: float32 [3072, 6144], P('gy', 'gx')
The draws below stay inside these ranges and needn't reach their ends.
All inputs are finite; a program needn't handle non-finite values.
Results may differ from the reference program's by a relative error of at most 0.013.
Values may be sent and summed in bfloat16 or wider, within the bound.
A program may use at most 128 MiB of HBM per device.

```python
import jax
import jax.numpy as jnp
from jax import lax

D = 3072
FF = 6144
TSTEPS = 1000
SEQ = 512
SAMPLES = 8
N_GX = 4
N_GY = 8


def set_ends(entries, rng, smallest, high):
    spot = [jax.random.randint(jax.random.fold_in(rng, axis), (), 0, length) for axis, length in enumerate(entries.shape)]
    main_axis = entries.shape.index(max(entries.shape))
    neighbour = spot[:main_axis] + [(spot[main_axis] + 1) % entries.shape[main_axis]] + spot[main_axis + 1:]
    return entries.at[tuple(spot)].set(smallest).at[tuple(neighbour)].set(high)


def level_of(key, dims, cuts, least, top_value):
    def one(axis_at, blocks):
        draws = jax.random.uniform(jax.random.fold_in(jax.random.fold_in(key, 6), axis_at), (blocks,), jnp.float32, least / len(cuts), top_value / len(cuts))
        return jnp.repeat(jnp.exp(draws), dims[axis_at] // blocks).reshape((-1,) + (1,) * (len(dims) - axis_at - 1))

    factor_of = one(*cuts[0])
    for cut in cuts[1:]:
        factor_of = factor_of * one(*cut)
    return factor_of


def normal_values(own_key, dims, scale, reach, shards=(), dtype=jnp.bfloat16):
    array = jax.random.normal(own_key, dims, jnp.float32) * scale
    if len(shards) > 0:
        array = level_of(own_key, dims, shards, -0.22, 0.18) * array
    return jnp.clip(array, min=-reach, max=reach).astype(dtype)


def setup_inputs(seed: int = 0) -> dict:
    seeds = jax.random.split(jax.random.key(seed), 12)
    return {
        "x_gen": normal_values(seeds[0], (SAMPLES, SEQ, D), 1.0, 6.0, ((0, 8), (1, 4))),
        "fresh_noise": normal_values(seeds[1], (SAMPLES, SEQ, D), 1.0, 6.0, ((0, 8), (1, 4))),
        "steps_t": set_ends(jax.random.randint(seeds[2], (SAMPLES,), 0, TSTEPS), jax.random.fold_in(seeds[2], 1), 0, TSTEPS - 1).astype(jnp.int32),
        "real_mod": normal_values(seeds[3], (SAMPLES, 2, D), 0.3, 2.5, ((0, 8),), jnp.float32),
        "real_w_up": normal_values(seeds[4], (D, FF), D ** -0.5, 0.109375, ((1, 4),)),
        "real_b_up": normal_values(seeds[5], (FF,), 0.5, 3.0, ((0, 4),), jnp.float32),
        "real_w_down": normal_values(seeds[6], (FF, D), FF ** -0.5, 0.078125, ((0, 4),)),
        "fake_mod": normal_values(seeds[7], (SAMPLES, 2, D), 0.3, 2.5, ((0, 8),), jnp.float32),
        "fake_w_up": normal_values(seeds[8], (D, FF), D ** -0.5, 0.109375, ((0, 8), (1, 4))),
        "fake_b_up": normal_values(seeds[9], (FF,), 0.5, 3.0, ((0, 4),), jnp.float32),
        "fake_w_down": normal_values(seeds[10], (FF, D), FF ** -0.5, 0.078125, ((0, 4), (1, 8))),
    }


def layer_norm(values):
    center = values - lax.optimization_barrier(jnp.mean(values, axis=-1, keepdims=True))
    spread = lax.optimization_barrier(jnp.mean(center * center, axis=-1, keepdims=True))
    return center * lax.rsqrt(spread + 1e-06)

def net_pred(normed, modulation, w_up, b_up, w_down):
    modulated = (normed * (1.0 + modulation[1]) + modulation[0]).astype(jnp.bfloat16)
    hidden = jax.nn.gelu(jnp.dot(modulated, w_up, preferred_element_type=jnp.float32) + b_up, approximate=True).astype(jnp.bfloat16)
    group_size = FF // N_GX
    partials = jnp.einsum('sgk,gkd->gsd', hidden.reshape(SEQ, N_GX, group_size).astype(jnp.float32), w_down.reshape(N_GX, group_size, D).astype(jnp.float32))
    partials = lax.optimization_barrier(partials.astype(jnp.bfloat16)).astype(jnp.float32)
    return (lax.optimization_barrier(jnp.sum(partials, axis=0)), hidden)

def reference(x_gen, fresh_noise, steps_t, real_mod, real_w_up, real_b_up, real_w_down, fake_mod, fake_w_up, fake_b_up, fake_w_down):
    loss_scale = float(SEQ * N_GY) ** (-0.5)

    def per_sample(grad_total, inputs):
        clean, drawn, step_index, modulation_real, modulation_fake = inputs
        noise_level = (step_index.astype(jnp.float32) + 1.0) / TSTEPS
        clean_f = clean.astype(jnp.float32)
        drawn_f = drawn.astype(jnp.float32)
        noised = ((1.0 - noise_level) * clean_f + noise_level * drawn_f).astype(jnp.bfloat16)
        target = (drawn_f - clean_f).astype(jnp.bfloat16)
        normed = layer_norm(noised.astype(jnp.float32))
        pred_real, unused_hidden = net_pred(normed, modulation_real, real_w_up, real_b_up, real_w_down)
        pred_fake, hidden_fake = net_pred(normed, modulation_fake, fake_w_up, fake_b_up, fake_w_down)
        dmd_grad = pred_fake - pred_real
        error_v = (pred_fake - target.astype(jnp.float32)).astype(jnp.bfloat16)
        partial_term = jnp.dot(error_v.T, hidden_fake, preferred_element_type=jnp.float32) * loss_scale
        partial_term = lax.optimization_barrier(partial_term.astype(jnp.bfloat16)).astype(jnp.float32)
        return (grad_total + partial_term, dmd_grad)
    grad_start = jnp.zeros((D, FF), jnp.float32)
    fake_grad, dmd_grad = lax.scan(per_sample, grad_start, (x_gen, fresh_noise, steps_t, real_mod, fake_mod))
    return (dmd_grad, fake_grad)
```

```python
import functools

import jax
import jax.numpy as jnp
from jax import lax
from jax.experimental import pallas as pl
from jax.experimental.pallas import tpu as pltpu
from jax.sharding import PartitionSpec as P

TSTEPS = 1000
BF = jnp.bfloat16
F32 = jnp.float32
MESH = pl.DeviceIdType.MESH
LANES = 128
TILE = 256
CHIPS = 4


def gelu(v):
    inner = 0.7978845608028654 * (v + 0.044715 * (v * v * v))
    return v * (0.5 * (1.0 + jnp.tanh(inner)))


def step_kernel(
    n,
    loss_scale,
    levels,
    x_hbm,
    noise_hbm,
    real_mod,
    real_up_hbm,
    real_bias,
    real_down_hbm,
    fake_mod,
    fake_up_hbm,
    fake_bias,
    fake_down_hbm,
    dmd,
    grad,
    up,
    real_up,
    real_down,
    fake_down,
    tokens,
    wide_in,
    real_hid,
    parts,
    recv,
    frecv,
    hid,
    err,
    target,
    goal,
    sent_pred,
    got_pred,
    total,
    local_sem,
    tile_sem,
    tok_send,
    tok_recv,
    rs_send,
    rs_recv,
    fs_send,
    fs_recv,
    up_send,
    up_recv,
    hid_send,
    hid_recv,
    goal_send,
    goal_recv,
    pred_send,
    pred_recv,
    err_send,
    err_recv,
):
    z = lax.axis_index("gx")
    g = lax.axis_index("gy")
    rows, width = x_hbm.shape[1:]
    hidden = real_up_hbm.shape[1]
    wide = fake_up_hbm.shape[0]
    piece = width // CHIPS
    core = lax.rem(g, 2)
    bit_x = lax.rem(g // 2, 2)
    bit_y = lax.rem(g // 4, 2)

    def peer(k):
        other = g
        if k & 1:
            other = other + (1 - 2 * core)
        if k & 2:
            other = other + 2 * (1 - 2 * bit_x)
        if k & 4:
            other = other + 4 * (1 - 2 * bit_y)
        return other

    def remote(src, dst, send, got, to):
        return pltpu.make_async_remote_copy(
            src_ref=src, dst_ref=dst, send_sem=send, recv_sem=got,
            device_id=to, device_id_type=MESH,
        )

    def cols(k, size):
        start = k * size
        if not isinstance(k, int):
            start = pl.multiple_of(start, LANES)
        return pl.ds(start, size)

    def row_block(k, size):
        return pl.ds(pl.multiple_of(k * size, LANES), size)

    def arrived(ref, sem):
        remote(ref, ref, local_sem.at[0], sem, (z, peer(1))).wait_recv()

    def left(ref, sem):
        remote(ref, ref, sem, local_sem.at[0], (z, peer(1))).wait_send()

    not_first = z > 0
    not_last = z < n - 1
    between = not_first & not_last

    load_x = pltpu.make_async_copy(x_hbm.at[0], parts.at[0], local_sem.at[0])
    load_noise = pltpu.make_async_copy(noise_hbm.at[0], parts.at[1], local_sem.at[1])
    load_own = pltpu.make_async_copy(fake_up_hbm, up.at[row_block(g, wide)], local_sem.at[2])
    load_real = pltpu.make_async_copy(real_up_hbm, real_up, local_sem.at[3])
    load_down = pltpu.make_async_copy(fake_down_hbm, fake_down, local_sem.at[4])
    load_x.start()
    load_noise.start()
    load_real.start()
    load_own.start()
    load_down.start()

    def load_tile(use):
        return pltpu.make_async_copy(
            real_down_hbm.at[:, cols(use % CHIPS, piece)], real_down.at[use % 2], tile_sem.at[use % 2]
        )

    load_tile(0).start()
    load_tile(1).start()

    barrier = pltpu.get_barrier_semaphore()
    for k in range(1, 8):
        pl.semaphore_signal(barrier, inc=1, device_id=(z, peer(k)), device_id_type=MESH)

    @pl.when(not_first)
    def _():
        pl.semaphore_signal(barrier, inc=1, device_id=(z - 1, g), device_id_type=MESH)

    @pl.when(not_last)
    def _():
        pl.semaphore_signal(barrier, inc=1, device_id=(z + 1, g), device_id_type=MESH)

    load_x.wait()
    load_noise.wait()

    def mix(i, carry):
        at = pl.ds(pl.multiple_of(i * 16, 16), 16)
        clean = parts[0, at, :].astype(F32)
        drawn = parts[1, at, :].astype(F32)
        tokens[z, at, :] = (levels[0] * clean + levels[1] * drawn).astype(BF)
        target[at, :] = (drawn - clean).astype(BF)
        return carry

    lax.fori_loop(0, rows // 16, mix, 0)
    goal[0] = target[:, cols(g, wide)]

    pl.semaphore_wait(barrier, 7 + jnp.minimum(z, 1) + jnp.minimum(n - 1 - z, 1))

    def token_copy(j, side):
        to = z + 1 if side == 0 else z - 1
        return remote(tokens.at[j], tokens.at[j], tok_send.at[side, j], tok_recv.at[j], (to, g))

    def up_copy(k, to):
        block = up.at[row_block(peer(k), wide)]
        source = fake_up_hbm if k == 0 else block
        return remote(source, block, up_send.at[k ^ to], up_recv.at[k ^ to], (z, peer(to)))

    def goal_copy(k):
        return remote(
            target.at[:, cols(peer(k), wide)], goal.at[k], goal_send.at[k], goal_recv.at[k], (z, peer(k))
        )

    @pl.when(not_last)
    def _():
        token_copy(z, 0).start()

    @pl.when(not_first)
    def _():
        token_copy(z, 1).start()

    for to in (2, 4, 6, 1):
        up_copy(0, to).start()

    def modulate(j, mod):
        def body(i, carry):
            at = pl.ds(pl.multiple_of(i * 16, 16), 16)
            v = tokens[j, at, :].astype(F32)
            center = v - jnp.mean(v, axis=-1, keepdims=True)
            spread = jnp.mean(center * center, axis=-1, keepdims=True)
            normed = center * lax.rsqrt(spread + 1e-06)
            wide_in[at, :] = (normed * (1.0 + mod[0, 1:2, :]) + mod[0, 0:1, :]).astype(BF)
            return carry

        lax.fori_loop(0, rows // 16, body, 0)

    def project(weights, bias, store):
        def body(t, carry):
            at = cols(t, TILE)
            pre = jnp.dot(wide_in[...], weights[:, at], preferred_element_type=F32) + bias[:, at]
            store(at, gelu(pre).astype(BF))
            return carry

        lax.fori_loop(0, hidden // TILE, body, 0)

    both = jnp.minimum(z, n - 1 - z)

    def arrival(r):
        if r == 0:
            return z
        near = z - (r + 1) // 2 if r % 2 == 1 else z + r // 2
        far = jnp.where(z > n - 1 - z, z - (r - both), z + (r - both))
        return jnp.where(r <= 2 * both, near, far)

    def part_copy(buf, got, send, recv_sem, j, f, side):
        at = cols(f, piece)
        if side == 0:
            to, slot = z + 1, j + 1
        else:
            to, slot = z - 1, j
        return remote(
            buf.at[j, :, at], got.at[slot, :, at], send.at[j, f], recv_sem.at[slot, f], (to, g)
        )

    def pass_tokens(r):
        j = arrival(r)

        @pl.when(between)
        def _():
            arrived(tokens.at[j], tok_recv.at[j])

            @pl.when(j < z)
            def _():
                token_copy(j, 0).start()

            @pl.when(j > z)
            def _():
                token_copy(j, 1).start()

    def real_chunk(r):
        j = arrival(r)
        if r > 0:
            @pl.when(jnp.logical_not(between))
            def _():
                arrived(tokens.at[j], tok_recv.at[j])

        modulate(j, real_mod)
        if r == 0:
            load_real.wait()

        def keep(at, value):
            real_hid[:, at] = value

        project(real_up, real_bias, keep)
        for f in range(CHIPS):
            use = r * CHIPS + f
            load_tile(use).wait()

            def down(t, carry):
                out = jnp.dot(
                    real_hid[...], real_down[use % 2, :, cols(t, TILE)], preferred_element_type=F32
                )
                parts[j, :, pl.ds(pl.multiple_of(f * piece + t * TILE, LANES), TILE)] = out.astype(BF)
                return carry

            lax.fori_loop(0, piece // TILE, down, 0)
            if use + 2 < n * CHIPS:
                load_tile(use + 2).start()
            if r > 0:
                @pl.when(z == 0)
                def _():
                    part_copy(parts, recv, rs_send, rs_recv, j, f, 0).start()

                @pl.when(z == n - 1)
                def _():
                    part_copy(parts, recv, rs_send, rs_recv, j, f, 1).start()

    def hid_copy(k, r, to):
        at = row_block(arrival(r), rows)
        return remote(
            hid.at[k, at], hid.at[k ^ to, at], hid_send.at[k ^ to, r], hid_recv.at[k ^ to, r],
            (z, peer(to)),
        )

    def fake_chunk(r):
        j = arrival(r)
        modulate(j, fake_mod)

        def keep(at, value):
            hid[0, row_block(j, rows), at] = value

        project(up, fake_bias, keep)
        for to in (2, 4, 1):
            hid_copy(0, r, to).start()

    def up_wait(k):
        arrived(up.at[row_block(peer(k), wide)], up_recv.at[k])

    real_chunk(0)
    for k in range(1, 8):
        goal_copy(k).start()
    for r in range(1, n - 1):
        if r % 2 == 1:
            for ahead in range(r, min(r + 2, n - 1)):
                pass_tokens(ahead)
        real_chunk(r)
        if r == 1:
            for k in (2, 4):
                up_wait(k)
                up_copy(k, 1).start()
    pass_tokens(n - 1)
    up_wait(6)
    up_copy(6, 1).start()
    load_own.wait()
    for k in (1, 3, 5, 7):
        up_wait(k)
    for r in range(n - 1):
        fake_chunk(r)
    real_chunk(n - 1)
    fake_chunk(n - 1)
    for r in range(n):
        hid_copy(0, r, 6).start()

    for j in range(n):
        @pl.when((j <= z) & not_last)
        def _():
            left(tokens.at[j], tok_send.at[0, j])

        @pl.when((j >= z) & not_first)
        def _():
            left(tokens.at[j], tok_send.at[1, j])

    def hid_wait(k):
        for r in range(n):
            arrived(hid.at[k, row_block(arrival(r), rows)], hid_recv.at[k, r])
            if k in (2, 4, 6):
                hid_copy(k, r, 1).start()

    load_down.wait()

    def fake_parts(c):
        for q in (0, 1):
            k = 2 * c + q

            def body(j, carry):
                out = jnp.dot(
                    hid[k, row_block(j, rows), :], fake_down[...], preferred_element_type=F32
                )
                tokens[j, :, cols(k, wide)] = out.astype(BF)
                return carry

            lax.fori_loop(0, n, body, 0)
        for e in range(n - 1, 0, -1):
            @pl.when(z == 0)
            def _():
                part_copy(tokens, frecv, fs_send, fs_recv, e, c, 0).start()

            @pl.when(z == n - 1)
            def _():
                part_copy(tokens, frecv, fs_send, fs_recv, n - 1 - e, c, 1).start()

    def part_wait(got, recv_sem, slot, f):
        arrived(got.at[slot, :, cols(f, piece)], recv_sem.at[slot, f])

    def relay(buf, got, send, recv_sem, f, right_owner, left_owner):
        at = cols(f, piece)
        for side, j in ((0, right_owner), (1, left_owner)):
            slot = j + 1 if side == 0 else j
            inside = (j > z) & (j < n) if side == 0 else (j >= 0) & (j < z)

            @pl.when(between & inside)
            def _():
                part_wait(got, recv_sem, slot, f)
                buf[j, :, at] = (buf[j, :, at].astype(F32) + got[slot, :, at].astype(F32)).astype(BF)
                part_copy(buf, got, send, recv_sem, j, f, side).start()

    def sum_own(buf, got, recv_sem, f):
        at = cols(f, piece)
        total[...] = buf[z, :, at].astype(F32)

        @pl.when(not_first)
        def _():
            part_wait(got, recv_sem, z + 1, f)
            total[...] += got[z + 1, :, at].astype(F32)

        @pl.when(not_last)
        def _():
            part_wait(got, recv_sem, z, f)
            total[...] += got[z, :, at].astype(F32)

    def real_sums():
        for t in range(3, 2 * n - 2):
            for f in range(CHIPS):
                relay(parts, recv, rs_send, rs_recv, f, t - z, 2 * (n - 1) - t - z)
        for f in range(CHIPS):
            sum_own(parts, recv, rs_recv, f)
            dmd[0, :, cols(f, piece)] = -total[...]

    def err_copy(j, c, side):
        to = z + 1 if side == 0 else z - 1
        block = err.at[j, :, cols(c, piece)]
        return remote(block, block, err_send.at[side, j, c], err_recv.at[j, c], (to, g))

    def pred_copy(k):
        return remote(
            sent_pred.at[k], got_pred.at[k], pred_send.at[k], pred_recv.at[k], (z, peer(k))
        )

    def fake_sums(c):
        for t in range(1, n - 1):
            relay(tokens, frecv, fs_send, fs_recv, c, n - 1 + z - t, t - (n - 1 - z))
        sum_own(tokens, frecv, fs_recv, c)
        for q in (0, 1):
            k = 2 * c + q
            if k > 0:
                arrived(goal.at[k], goal_recv.at[k])
            pred = total[:, q * wide:(q + 1) * wide]
            sent_pred[k] = pred.astype(BF)
            err[z, :, cols(k, wide)] = (pred - goal[k].astype(F32)).astype(BF)

        @pl.when(not_last)
        def _():
            err_copy(z, c, 0).start()

        @pl.when(not_first)
        def _():
            err_copy(z, c, 1).start()

        for q in (0, 1):
            if 2 * c + q > 0:
                pred_copy(2 * c + q).start()

    def gradient(c):
        for d in range(1, n):
            @pl.when(z - d >= 0)
            def _():
                arrived(err.at[z - d, :, cols(c, piece)], err_recv.at[z - d, c])

                @pl.when(not_last)
                def _():
                    err_copy(z - d, c, 0).start()

            @pl.when(z + d <= n - 1)
            def _():
                arrived(err.at[z + d, :, cols(c, piece)], err_recv.at[z + d, c])

                @pl.when(not_first)
                def _():
                    err_copy(z + d, c, 1).start()

        def body(t, carry):
            at = cols(t, TILE)
            out = jnp.zeros((wide, TILE), F32) if c == 0 else grad[:, at]
            for q in (0, 1):
                k = 2 * c + q
                errors = err[:, :, k * wide:(k + 1) * wide].reshape(n * rows, wide)
                out = out + lax.dot_general(
                    errors, hid[k, :, at], (((0,), (0,)), ((), ())), preferred_element_type=F32
                )
            if c == CHIPS - 1:
                out = out * loss_scale
            grad[:, at] = out
            return carry

        lax.fori_loop(0, hidden // TILE, body, 0)

    hid_wait(1)
    fake_parts(0)
    real_sums()
    hid_wait(2)
    hid_wait(3)
    fake_parts(1)
    fake_sums(0)
    hid_wait(4)
    hid_wait(5)
    fake_parts(2)
    fake_sums(1)
    gradient(0)
    hid_wait(6)
    hid_wait(7)
    fake_parts(3)
    fake_sums(2)
    gradient(1)
    fake_sums(3)
    gradient(2)
    gradient(3)

    dmd[0, :, cols(g, wide)] += sent_pred[0].astype(F32)
    for k in range(1, 8):
        arrived(got_pred.at[k], pred_recv.at[k])
        dmd[0, :, cols(peer(k), wide)] += got_pred[k].astype(F32)

    for k in range(1, 8):
        left(fake_up_hbm, up_send.at[k])
        for r in range(n):
            left(hid.at[0, row_block(r, rows)], hid_send.at[k, r])
        left(goal.at[k], goal_send.at[k])
        left(sent_pred.at[k], pred_send.at[k])
    for j in range(n):
        for f in range(CHIPS):
            @pl.when(j != z)
            def _():
                left(parts.at[j, :, cols(f, piece)], rs_send.at[j, f])
                left(tokens.at[j, :, cols(f, piece)], fs_send.at[j, f])

            @pl.when((j <= z) & not_last)
            def _():
                left(err.at[j, :, cols(f, piece)], err_send.at[0, j, f])

            @pl.when((j >= z) & not_first)
            def _():
                left(err.at[j, :, cols(f, piece)], err_send.at[1, j, f])


def one_kernel(
    x_gen, fresh_noise, steps_t, real_mod, real_w_up, real_b_up, real_w_down,
    fake_mod, fake_w_up, fake_b_up, fake_w_down,
):
    n = lax.axis_size("gx")
    rows, width = x_gen.shape[1:]
    hidden = real_w_up.shape[1]
    wide = fake_w_up.shape[0]
    piece = width // CHIPS
    level = (steps_t[0].astype(F32) + 1.0) / TSTEPS
    levels = jnp.stack([1.0 - level, level])
    loss_scale = float(lax.axis_size("gy") * n * rows) ** (-0.5)
    vmem = pl.BlockSpec(memory_space=pltpu.VMEM)
    held = pl.BlockSpec(memory_space=pl.ANY)
    dma = pltpu.SemaphoreType.DMA
    flops = 10 * n * rows * width * hidden
    return pl.pallas_call(
        functools.partial(step_kernel, n, loss_scale),
        out_shape=(
            jax.ShapeDtypeStruct((1, rows, width), F32),
            jax.ShapeDtypeStruct((wide, hidden), F32),
        ),
        in_specs=[
            pl.BlockSpec(memory_space=pltpu.SMEM), held, held,
            vmem, held, vmem, held,
            vmem, held, vmem, held,
        ],
        out_specs=(vmem, vmem),
        scratch_shapes=[
            pltpu.VMEM((width, hidden), BF),
            pltpu.VMEM((width, hidden), BF),
            pltpu.VMEM((2, hidden, piece), BF),
            pltpu.VMEM((hidden, wide), BF),
            pltpu.VMEM((n, rows, width), BF),
            pltpu.VMEM((rows, width), BF),
            pltpu.VMEM((rows, hidden), BF),
            pltpu.VMEM((n, rows, width), BF),
            pltpu.VMEM((n + 1, rows, width), BF),
            pltpu.VMEM((n + 1, rows, width), BF),
            pltpu.VMEM((8, n * rows, hidden), BF),
            pltpu.VMEM((n, rows, width), BF),
            pltpu.VMEM((rows, width), BF),
            pltpu.VMEM((8, rows, wide), BF),
            pltpu.VMEM((8, rows, wide), BF),
            pltpu.VMEM((8, rows, wide), BF),
            pltpu.VMEM((rows, piece), F32),
            dma((5,)),
            dma((2,)),
            dma((2, n)),
            dma((n,)),
            dma((n, CHIPS)),
            dma((n + 1, CHIPS)),
            dma((n, CHIPS)),
            dma((n + 1, CHIPS)),
            dma((8,)),
            dma((8,)),
            dma((8, n)),
            dma((8, n)),
            dma((8,)),
            dma((8,)),
            dma((8,)),
            dma((8,)),
            dma((2, n, CHIPS)),
            dma((n, CHIPS)),
        ],
        compiler_params=pltpu.CompilerParams(
            collective_id=0, has_side_effects=True, vmem_limit_bytes=67043328
        ),
        cost_estimate=pl.CostEstimate(flops=flops, bytes_accessed=flops // 512, transcendentals=0),
    )(
        levels, x_gen, fresh_noise,
        real_mod, real_w_up, real_b_up[None], real_w_down,
        fake_mod, fake_w_up, fake_b_up[None], fake_w_down,
    )


def layer_norm(values):
    center = values - jnp.mean(values, axis=-1, keepdims=True)
    spread = jnp.mean(center * center, axis=-1, keepdims=True)
    return center * lax.rsqrt(spread + 1e-06)


def halves(block):
    cut = block.shape[0] // 2
    return [block[:cut], block[cut:]]


def add(a, b):
    return a.astype(F32) + b.astype(F32)


def ring_shift(value, step):
    n = lax.axis_size("gx")
    return lax.ppermute(value, "gx", [(i, (i + step) % n) for i in range(n)])


def flip(value, bit):
    n = lax.axis_size("gy")
    return lax.ppermute(value, "gy", [(i, i ^ bit) for i in range(n)])


def ring_gather(own):
    n = lax.axis_size("gx")
    blocks = {0: own}
    if n == 1:
        return blocks
    far = n // 2
    for d in range(1, far):
        blocks[n - d] = ring_shift(blocks[(n - d + 1) % n], 1)
        blocks[d] = ring_shift(blocks[d - 1], -1)
    first = ring_shift(halves(blocks[(n - far + 1) % n])[0], 1)
    second = ring_shift(halves(blocks[far - 1])[1], -1)
    blocks[far] = jnp.concatenate([first, second], axis=0)
    return blocks


def ring_scatter(parts):
    n = lax.axis_size("gx")
    cut = [halves(part) for part in parts]
    total = [half.astype(F32) for half in cut[0]]
    far = n // 2
    for half in (0, 1):
        for step in (1, -1):
            start = far if (half == 0) == (step == 1) else far - 1
            if start < 1:
                continue
            running = cut[(step * start) % n][half]
            for d in range(start, 0, -1):
                got = ring_shift(running, step)
                if d > 1:
                    running = add(cut[(step * (d - 1)) % n][half], got).astype(BF)
                else:
                    total[half] = total[half] + got.astype(F32)
    return jnp.concatenate(total, axis=0)


def route(k):
    return k & -k, 1 << (k.bit_length() - 1)


def chip_offsets(n):
    return sorted(range(2, n, 2), key=lambda k: (bin(k).count("1"), k))


def plane_gather(own):
    n = lax.axis_size("gy")
    blocks = {0: own}
    for k in chip_offsets(n):
        low, high = route(k)
        if low == high:
            blocks[k] = flip(own, k)
        else:
            first = flip(halves(blocks[k ^ low])[0], low)
            second = flip(halves(blocks[k ^ high])[1], high)
            blocks[k] = jnp.concatenate([first, second], axis=0)
    for k in range(0, n, 2):
        blocks[k + 1] = flip(blocks[k], 1)
    return blocks


def plane_scatter(parts):
    n = lax.axis_size("gy")
    held = {k: halves(add(parts[k], flip(parts[k + 1], 1))) for k in range(0, n, 2)}
    for k in reversed(chip_offsets(n)):
        low, high = route(k)
        for half, bit in ((0, low), (1, high)):
            got = flip(held[k][half].astype(BF), bit)
            held[k ^ bit][half] = held[k ^ bit][half] + got.astype(F32)
    return jnp.concatenate(held[0], axis=0)


def plain(
    x_gen,
    fresh_noise,
    steps_t,
    real_mod,
    real_w_up,
    real_b_up,
    real_w_down,
    fake_mod,
    fake_w_up,
    fake_b_up,
    fake_w_down,
):
    n_gx, n_gy = lax.axis_size("gx"), lax.axis_size("gy")
    me = lax.axis_index("gy")
    noise_level = (steps_t[0].astype(F32) + 1.0) / TSTEPS
    clean_f = x_gen[0].astype(F32)
    drawn_f = fresh_noise[0].astype(F32)
    noised = ((1.0 - noise_level) * clean_f + noise_level * drawn_f).astype(BF)
    target = (drawn_f - clean_f).astype(BF)
    own_rows, width = noised.shape
    wide = fake_w_up.shape[0]

    up_blocks = plane_gather(fake_w_up)
    tokens = ring_gather(noised)
    down_blocks = plane_gather(fake_w_down)

    def columns(array, k):
        return lax.dynamic_slice_in_dim(array, (me ^ k) * wide, wide, axis=1)

    noised_all = jnp.concatenate([tokens[j] for j in range(n_gx)], axis=0)
    normed = layer_norm(noised_all.astype(F32))
    real_in = (normed * (1.0 + real_mod[0, 1]) + real_mod[0, 0]).astype(BF)
    fake_in = (normed * (1.0 + fake_mod[0, 1]) + fake_mod[0, 0]).astype(BF)
    real_in, fake_in = lax.optimization_barrier((real_in, fake_in))
    real_hidden = jax.nn.gelu(
        jnp.dot(real_in, real_w_up, preferred_element_type=F32) + real_b_up, approximate=True
    ).astype(BF)
    real_part = jnp.dot(real_hidden, real_w_down, preferred_element_type=F32).astype(BF)
    real_rows = ring_scatter([real_part[j * own_rows:(j + 1) * own_rows] for j in range(n_gx)])

    fake_pre = fake_b_up[None]
    for k in range(n_gy):
        fake_pre = fake_pre + jnp.dot(
            columns(fake_in, k), up_blocks[k], preferred_element_type=F32
        )
    fake_hidden = jax.nn.gelu(fake_pre, approximate=True).astype(BF)

    loss_scale = float(n_gy * n_gx * own_rows) ** (-0.5)
    dmd_grad = jnp.zeros((own_rows, width), F32)
    products = {}
    for k in range(0, n_gy, 2):
        pair = jnp.concatenate(
            [
                jnp.dot(fake_hidden, down_blocks[i], preferred_element_type=F32).astype(BF)
                for i in (k, k + 1)
            ],
            axis=1,
        )
        pred = ring_scatter([pair[j * own_rows:(j + 1) * own_rows] for j in range(n_gx)])
        goal = jnp.concatenate([columns(target, i) for i in (k, k + 1)], axis=1)
        error = ring_gather((pred - goal.astype(F32)).astype(BF))
        error_all = jnp.concatenate([error[j] for j in range(n_gx)], axis=0)
        for i in (0, 1):
            part = slice(i * wide, (i + 1) * wide)
            dmd_grad = lax.dynamic_update_slice_in_dim(
                dmd_grad, pred[:, part], (me ^ (k + i)) * wide, axis=1
            )
            product = lax.dot_general(
                error_all[:, part],
                fake_hidden,
                (((0,), (0,)), ((), ())),
                preferred_element_type=F32,
            )
            products[k + i] = (product * loss_scale).astype(BF)
    fake_grad = plane_scatter(products)
    return ((dmd_grad - real_rows)[None], fake_grad)


def shards(*arrays):
    n_gx, n_gy = lax.axis_size("gx"), lax.axis_size("gy")
    wide, hidden = arrays[8].shape
    fits = n_gy == 2 * CHIPS and n_gx >= 3 and wide % LANES == 0 and hidden % TILE == 0
    return one_kernel(*arrays) if fits else plain(*arrays)


def solution(mesh):
    return jax.shard_map(
        shards,
        mesh=mesh,
        in_specs=(
            P("gy", "gx", None),
            P("gy", "gx", None),
            P("gy"),
            P("gy", None, None),
            P(None, "gx"),
            P("gx"),
            P("gx", None),
            P("gy", None, None),
            P("gy", "gx"),
            P("gx"),
            P("gx", "gy"),
        ),
        out_specs=(P("gy", "gx", None), P("gy", "gx")),
        check_vma=False,
    )
```

```python
import functools

import jax
import jax.numpy as jnp
from jax import lax
from jax.experimental import pallas as pl
from jax.experimental.pallas import tpu as pltpu
from jax.sharding import PartitionSpec as P

TSTEPS = 1000
BF = jnp.bfloat16
F32 = jnp.float32
MESH = pl.DeviceIdType.MESH
LANES = 128
TILE = 256
CHIPS = 4


def gelu(v):
    inner = 0.7978845608028654 * (v + 0.044715 * (v * v * v))
    return v * (0.5 * (1.0 + jnp.tanh(inner)))


def step_kernel(
    n,
    loss_scale,
    steps,
    x_hbm,
    noise_hbm,
    real_mod,
    real_up_hbm,
    real_bias_hbm,
    real_down_hbm,
    fake_mod,
    fake_up_hbm,
    fake_bias_hbm,
    fake_down_hbm,
    dmd_hbm,
    grad_hbm,
    dmd,
    grad,
    real_bias,
    fake_bias,
    up,
    real_up,
    real_down,
    fake_down,
    tokens,
    wide_in,
    real_hid,
    parts,
    recv,
    frecv,
    hid,
    target,
    goal,
    sent_pred,
    got_pred,
    total,
    local_sem,
    tile_sem,
    tok_send,
    tok_recv,
    rs_send,
    rs_recv,
    fs_send,
    fs_recv,
    up_send,
    up_recv,
    hid_send,
    hid_recv,
    goal_send,
    goal_recv,
    pred_send,
    pred_recv,
    out_sem,
    err_send,
    err_recv,
):
    z = lax.axis_index("gx")
    g = lax.axis_index("gy")
    rows, width = x_hbm.shape[1:]
    hidden = real_up_hbm.shape[1]
    wide = fake_up_hbm.shape[0]
    piece = width // CHIPS
    core = lax.rem(g, 2)
    bit_x = lax.rem(g // 2, 2)
    bit_y = lax.rem(g // 4, 2)

    def peer(k):
        other = g
        if k & 1:
            other = other + (1 - 2 * core)
        if k & 2:
            other = other + 2 * (1 - 2 * bit_x)
        if k & 4:
            other = other + 4 * (1 - 2 * bit_y)
        return other

    def remote(src, dst, send, got, to):
        return pltpu.make_async_remote_copy(
            src_ref=src, dst_ref=dst, send_sem=send, recv_sem=got,
            device_id=to, device_id_type=MESH,
        )

    def cols(k, size):
        start = k * size
        if not isinstance(k, int):
            start = pl.multiple_of(start, LANES)
        return pl.ds(start, size)

    def row_block(k, size):
        return pl.ds(pl.multiple_of(k * size, LANES), size)

    def arrived(ref, sem):
        remote(ref, ref, local_sem.at[0], sem, (z, peer(1))).wait_recv()

    def left(ref, sem):
        remote(ref, ref, sem, local_sem.at[0], (z, peer(1))).wait_send()

    not_first = z > 0
    not_last = z < n - 1
    between = not_first & not_last

    barrier = pltpu.get_barrier_semaphore()
    for k in range(1, 8):
        pl.semaphore_signal(barrier, inc=1, device_id=(z, peer(k)), device_id_type=MESH)

    @pl.when(not_first)
    def _():
        pl.semaphore_signal(barrier, inc=1, device_id=(z - 1, g), device_id_type=MESH)

    @pl.when(not_last)
    def _():
        pl.semaphore_signal(barrier, inc=1, device_id=(z + 1, g), device_id_type=MESH)

    load_x = pltpu.make_async_copy(x_hbm.at[0], parts.at[0], local_sem.at[0])
    load_noise = pltpu.make_async_copy(noise_hbm.at[0], parts.at[1], local_sem.at[1])
    load_own = pltpu.make_async_copy(fake_up_hbm, up.at[row_block(g, wide)], local_sem.at[2])
    load_real = pltpu.make_async_copy(real_up_hbm, real_up, local_sem.at[3])
    load_down = pltpu.make_async_copy(fake_down_hbm, fake_down, local_sem.at[4])
    load_real_bias = pltpu.make_async_copy(real_bias_hbm, real_bias.at[0], local_sem.at[5])
    load_fake_bias = pltpu.make_async_copy(fake_bias_hbm, fake_bias.at[0], local_sem.at[6])
    load_x.start()
    load_noise.start()
    load_real_bias.start()
    load_fake_bias.start()
    load_real.start()

    def load_tile(f):
        return pltpu.make_async_copy(
            real_down_hbm.at[:, cols(f, piece)], real_down.at[:, cols(f, piece)], tile_sem.at[f]
        )

    for f in range(CHIPS):
        load_tile(f).start()
    load_own.start()
    load_down.start()

    def token_copy(j, side):
        to = z + 1 if side == 0 else z - 1
        return remote(tokens.at[j], tokens.at[j], tok_send.at[side, j], tok_recv.at[j], (to, g))

    def up_copy(k, to):
        block = up.at[row_block(peer(k), wide)]
        source = fake_up_hbm if k == 0 else block
        return remote(source, block, up_send.at[k ^ to], up_recv.at[k ^ to], (z, peer(to)))

    def half_copy(array, send, got, row, size, k, to):
        half = size // 2
        block = array.at[pl.ds(pl.multiple_of(row + (0 if k == 2 else half), 32), half)]
        return remote(block, block, send.at[6 if k == 2 else 0], got.at[6], (z, peer(to)))

    def pass_up(k):
        up_wait(k)
        if k != 6:
            half_copy(up, up_send, up_recv, peer(k) * wide, wide, k, 6 - k).start()
        up_copy(k, 1).start()

    def goal_copy(k):
        return remote(
            target.at[:, cols(peer(k), wide)], goal.at[k], goal_send.at[k], goal_recv.at[k], (z, peer(k))
        )

    pl.semaphore_wait(barrier, 7 + jnp.minimum(z, 1) + jnp.minimum(n - 1 - z, 1))
    for to in (2, 4, 1):
        up_copy(0, to).start()

    load_x.wait()
    load_noise.wait()
    level = (jnp.full((1, LANES), steps[0].astype(F32), F32) + 1.0) / TSTEPS
    level = level[:, :1]

    def mix(i, carry):
        at = pl.ds(pl.multiple_of(i * 16, 16), 16)
        clean = parts[0, at, :].astype(F32)
        drawn = parts[1, at, :].astype(F32)
        tokens[z, at, :] = ((1.0 - level) * clean + level * drawn).astype(BF)
        target[at, :] = (drawn - clean).astype(BF)
        return carry

    quarter = rows // 4
    for part in range(4):
        lax.fori_loop(part * quarter // 16, (part + 1) * quarter // 16, mix, 0)
        block = tokens.at[z, pl.ds(part * quarter, quarter)]

        @pl.when(not_last)
        def _():
            remote(block, block, tok_send.at[0, z], tok_recv.at[z], (z + 1, g)).start()

        @pl.when(not_first)
        def _():
            remote(block, block, tok_send.at[1, z], tok_recv.at[z], (z - 1, g)).start()

    goal[0] = target[:, cols(g, wide)]

    def modulate(j, mod):
        def body(i, carry):
            at = pl.ds(pl.multiple_of(i * 16, 16), 16)
            v = tokens[j, at, :].astype(F32)
            center = v - jnp.mean(v, axis=-1, keepdims=True)
            spread = jnp.mean(center * center, axis=-1, keepdims=True)
            normed = center * lax.rsqrt(spread + 1e-06)
            wide_in[at, :] = (normed * (1.0 + mod[0, 1:2, :]) + mod[0, 0:1, :]).astype(BF)
            return carry

        lax.fori_loop(0, rows // 16, body, 0)

    def project(weights, bias, store):
        def body(t, carry):
            at = cols(t, TILE)
            pre = jnp.dot(wide_in[...], weights[:, at], preferred_element_type=F32) + bias[:, at]
            store(at, gelu(pre).astype(BF))
            return carry

        lax.fori_loop(0, hidden // TILE, body, 0)

    both = jnp.minimum(z, n - 1 - z)

    def arrival(r):
        if r == 0:
            return z
        near = z - (r + 1) // 2 if r % 2 == 1 else z + r // 2
        far = jnp.where(z > n - 1 - z, z - (r - both), z + (r - both))
        return jnp.where(r <= 2 * both, near, far)

    def part_copy(buf, got, send, recv_sem, j, f, side):
        at = cols(f, piece)
        if side == 0:
            to, slot = z + 1, j + 1
        else:
            to, slot = z - 1, j
        return remote(
            buf.at[j, :, at], got.at[slot, :, at], send.at[j, f], recv_sem.at[slot, f], (to, g)
        )

    def pass_tokens(r):
        j = arrival(r)

        @pl.when(between)
        def _():
            arrived(tokens.at[j], tok_recv.at[j])

            @pl.when(j < z)
            def _():
                token_copy(j, 0).start()

            @pl.when(j > z)
            def _():
                token_copy(j, 1).start()

    def real_chunk(r):
        j = arrival(r)
        if r > 0:
            @pl.when(jnp.logical_not(between))
            def _():
                arrived(tokens.at[j], tok_recv.at[j])

        modulate(j, real_mod)
        if r == 0:
            load_real_bias.wait()
            load_real.wait()

        def keep(at, value):
            real_hid[:, at] = value

        project(real_up, real_bias, keep)
        for f in range(CHIPS):
            if r == 0:
                load_tile(f).wait()

            def down(t, carry):
                at = pl.ds(pl.multiple_of(f * piece + t * TILE, LANES), TILE)
                out = jnp.dot(real_hid[...], real_down[:, at], preferred_element_type=F32)
                parts[j, :, at] = out.astype(BF)
                return carry

            lax.fori_loop(0, piece // TILE, down, 0)
            if r > 0:
                @pl.when(z == 0)
                def _():
                    part_copy(parts, recv, rs_send, rs_recv, j, f, 0).start()

                @pl.when(z == n - 1)
                def _():
                    part_copy(parts, recv, rs_send, rs_recv, j, f, 1).start()

    def hid_copy(k, r, to):
        at = row_block(arrival(r), rows)
        return remote(
            hid.at[k, at], hid.at[k ^ to, at], hid_send.at[k ^ to, r], hid_recv.at[k ^ to, r],
            (z, peer(to)),
        )

    def fake_chunk(r):
        j = arrival(r)
        modulate(j, fake_mod)

        def keep(at, value):
            hid[0, row_block(j, rows), at] = value

        project(up, fake_bias, keep)
        for to in (2, 4, 1):
            hid_copy(0, r, to).start()

    def up_wait(k):
        arrived(up.at[row_block(peer(k), wide)], up_recv.at[k])

    def tokens_left():
        for j in range(n):
            @pl.when((j <= z) & not_last)
            def _():
                left(tokens.at[j], tok_send.at[0, j])

            @pl.when((j >= z) & not_first)
            def _():
                left(tokens.at[j], tok_send.at[1, j])

    def up_left():
        for k in range(8):
            parting = 2 if k in (0, 6) else 1
            left(fake_up_hbm.at[pl.ds(0, wide // parting)], up_send.at[k])

    def hid_wait(k):
        for r in range(n):
            start = pl.multiple_of(arrival(r) * rows, LANES)
            arrived(hid.at[k, pl.ds(start, rows)], hid_recv.at[k, r])
            if k in (2, 4):
                half = rows // 2
                at = pl.ds(pl.multiple_of(start + (0 if k == 2 else half), 16), half)
                remote(
                    hid.at[k, at], hid.at[6, at], hid_send.at[6 if k == 2 else 0, r], hid_recv.at[6, r],
                    (z, peer(6 - k)),
                ).start()
            if k in (2, 4, 6):
                hid_copy(k, r, 1).start()

    def fake_parts(c):
        for q in (0, 1):
            k = 2 * c + q

            def body(j, carry):
                out = jnp.dot(
                    hid[k, row_block(j, rows), :], fake_down[...], preferred_element_type=F32
                )
                tokens[j, :, cols(k, wide)] = out.astype(BF)
                return carry

            lax.fori_loop(0, n, body, 0)
        for e in range(n - 1, 0, -1):
            @pl.when(z == 0)
            def _():
                part_copy(tokens, frecv, fs_send, fs_recv, e, c, 0).start()

            @pl.when(z == n - 1)
            def _():
                part_copy(tokens, frecv, fs_send, fs_recv, n - 1 - e, c, 1).start()

    def part_wait(got, recv_sem, slot, f):
        arrived(got.at[slot, :, cols(f, piece)], recv_sem.at[slot, f])

    def relay(buf, got, send, recv_sem, f, right_owner, left_owner):
        at = cols(f, piece)
        for side, j in ((0, right_owner), (1, left_owner)):
            slot = j + 1 if side == 0 else j
            inside = (j > z) & (j < n) if side == 0 else (j >= 0) & (j < z)

            @pl.when(between & inside)
            def _():
                part_wait(got, recv_sem, slot, f)
                buf[j, :, at] = (buf[j, :, at].astype(F32) + got[slot, :, at].astype(F32)).astype(BF)
                part_copy(buf, got, send, recv_sem, j, f, side).start()

    def sum_own(buf, got, recv_sem, f):
        at = cols(f, piece)
        total[...] = buf[z, :, at].astype(F32)

        @pl.when(not_first)
        def _():
            part_wait(got, recv_sem, z + 1, f)
            total[...] += got[z + 1, :, at].astype(F32)

        @pl.when(not_last)
        def _():
            part_wait(got, recv_sem, z, f)
            total[...] += got[z, :, at].astype(F32)

    def relay_real(t, f):
        relay(parts, recv, rs_send, rs_recv, f, t - z, 2 * (n - 1) - t - z)

    def own_real():
        for f in range(CHIPS):
            sum_own(parts, recv, rs_recv, f)
            dmd[0, :, cols(f, piece)] = -total[...]

    def relay_fake(c, t):
        relay(tokens, frecv, fs_send, fs_recv, c, n - 1 + z - t, t - (n - 1 - z))

    def err_block(j, c):
        row = ((c // 2) * n + j) * rows
        return up.at[pl.ds(pl.multiple_of(row, LANES), rows), cols(c % 2, piece)]

    def err_copy(j, c, side):
        to = z + 1 if side == 0 else z - 1
        block = err_block(j, c)
        return remote(block, block, err_send.at[side, j, c], err_recv.at[j, c], (to, g))

    def pred_copy(k):
        return remote(
            sent_pred.at[k], got_pred.at[k], pred_send.at[k], pred_recv.at[k], (z, peer(k))
        )

    def own_fake(c):
        sum_own(tokens, frecv, fs_recv, c)
        for q in (0, 1):
            k = 2 * c + q
            if k > 0:
                arrived(goal.at[k], goal_recv.at[k])
            pred = total[:, q * wide:(q + 1) * wide]
            sent_pred[k] = pred.astype(BF)
            err_block(z, c)[:, q * wide:(q + 1) * wide] = (pred - goal[k].astype(F32)).astype(BF)

        @pl.when(not_last)
        def _():
            err_copy(z, c, 0).start()

        @pl.when(not_first)
        def _():
            err_copy(z, c, 1).start()

        for q in (0, 1):
            if 2 * c + q > 0:
                pred_copy(2 * c + q).start()

    def pass_side(c, d, side):
        j = z - d if side == 0 else z + d
        arrived(err_block(j, c), err_recv.at[j, c])
        err_copy(j, c, side).start()

    def pass_errors(c, d, inner):
        low = 2 * z < n

        @pl.when(between & (low if inner else jnp.logical_not(low)) & (z + d <= n - 1))
        def _():
            pass_side(c, d, 1)

        @pl.when(between & (jnp.logical_not(low) if inner else low) & (z - d >= 0))
        def _():
            pass_side(c, d, 0)

    def grad_out(t):
        return pltpu.make_async_copy(
            grad.at[:, cols(t, TILE)], grad_hbm.at[:, cols(t, TILE)], out_sem.at[t + 1]
        )

    def add_preds(c):
        for k in (2 * c, 2 * c + 1):
            if k > 0:
                arrived(got_pred.at[k], pred_recv.at[k])
            got = sent_pred[0] if k == 0 else got_pred[k]
            dmd[0, :, cols(peer(k), wide)] += got.astype(F32)

    def gradient(c):
        for j in range(n):
            @pl.when(jnp.logical_not(between) & (j != z))
            def _():
                arrived(err_block(j, c), err_recv.at[j, c])

        def body(t, carry):
            at = cols(t, TILE)
            out = jnp.zeros((wide, TILE), F32) if c == 0 else grad[:, at]
            for q in (0, 1):
                k = 2 * c + q
                row, col = (c // 2) * n * rows, (c % 2) * piece + q * wide
                errors = up[row:row + n * rows, col:col + wide]
                out = out + lax.dot_general(
                    errors, hid[k, :, at], (((0,), (0,)), ((), ())), preferred_element_type=F32
                )
            if c == CHIPS - 1:
                out = out * loss_scale
            grad[:, at] = out
            if c == CHIPS - 1:
                grad_out(t).start()
            return carry

        lax.fori_loop(0, hidden // TILE, body, 0)

    def rest_errors(c):
        pass_errors(c, 1, False)
        for d in range(2, n - 1):
            pass_errors(c, d, True)
            pass_errors(c, d, False)

    hops = range(3, 2 * n - 2)
    turns = range(1, n - 1)
    real_chunk(0)
    for r in range(1, n - 1):
        if r % 2 == 1:
            for ahead in range(r, min(r + 2, n - 1)):
                pass_tokens(ahead)
        real_chunk(r)
        if r == 1:
            pass_up(2)
            pass_up(4)
            for k in range(1, 8):
                goal_copy(k).start()
    pass_tokens(n - 1)
    pass_up(6)
    load_own.wait()
    load_fake_bias.wait()
    load_down.wait()
    for k in (1, 3, 5, 7):
        up_wait(k)
    for r in range(n - 2):
        fake_chunk(r)
    for f in range(CHIPS - 1):
        relay_real(hops[0], f)
    real_chunk(n - 1)
    relay_real(hops[0], CHIPS - 1)
    fake_chunk(n - 2)
    for t in hops[1:-1]:
        for f in range(CHIPS // 2):
            relay_real(t, f)
    fake_chunk(n - 1)
    for t in hops[1:-1]:
        for f in range(CHIPS // 2, CHIPS):
            relay_real(t, f)
    tokens_left()
    up_left()
    hid_wait(1)
    fake_parts(0)
    for f in range(CHIPS):
        if len(hops) > 1:
            relay_real(hops[-1], f)
    relay_fake(0, 1)
    hid_wait(2)
    hid_wait(3)
    fake_parts(1)
    for t in turns[1:]:
        relay_fake(0, t)
    own_fake(0)
    relay_fake(1, 1)
    pass_errors(0, 1, True)
    hid_wait(4)
    hid_wait(5)
    fake_parts(2)
    for t in turns[1:]:
        relay_fake(1, t)
    own_fake(1)
    rest_errors(0)
    relay_fake(2, 1)
    pass_errors(1, 1, True)
    hid_wait(6)
    hid_wait(7)
    fake_parts(3)
    for t in turns[1:]:
        relay_fake(2, t)
    own_fake(2)
    rest_errors(1)
    relay_fake(3, 1)
    pass_errors(2, 1, True)
    for t in turns[1:]:
        relay_fake(3, t)
    own_fake(3)
    own_real()
    gradient(0)
    rest_errors(2)
    pass_errors(3, 1, True)
    gradient(1)
    add_preds(0)
    add_preds(1)
    rest_errors(3)
    gradient(2)
    add_preds(2)
    add_preds(3)
    dmd_out = pltpu.make_async_copy(dmd, dmd_hbm, out_sem.at[0])
    dmd_out.start()
    gradient(3)

    for k in range(8):
        parting = 2 if k in (0, 6) else 1
        for r in range(n):
            left(hid.at[0, pl.ds(0, rows // parting)], hid_send.at[k, r])
    for k in range(1, 8):
        left(goal.at[k], goal_send.at[k])
        left(sent_pred.at[k], pred_send.at[k])
    for j in range(n):
        for f in range(CHIPS):
            @pl.when(j != z)
            def _():
                left(parts.at[j, :, cols(f, piece)], rs_send.at[j, f])
                left(tokens.at[j, :, cols(f, piece)], fs_send.at[j, f])

            @pl.when((j <= z) & not_last)
            def _():
                left(err_block(j, f), err_send.at[0, j, f])

            @pl.when((j >= z) & not_first)
            def _():
                left(err_block(j, f), err_send.at[1, j, f])
    for t in range(hidden // TILE):
        grad_out(t).wait()
    dmd_out.wait()


def one_kernel(
    x_gen, fresh_noise, steps_t, real_mod, real_w_up, real_b_up, real_w_down,
    fake_mod, fake_w_up, fake_b_up, fake_w_down,
):
    n = lax.axis_size("gx")
    rows, width = x_gen.shape[1:]
    hidden = real_w_up.shape[1]
    wide = fake_w_up.shape[0]
    piece = width // CHIPS
    loss_scale = float(lax.axis_size("gy") * n * rows) ** (-0.5)
    vmem = pl.BlockSpec(memory_space=pltpu.VMEM)
    held = pl.BlockSpec(memory_space=pl.ANY)
    dma = pltpu.SemaphoreType.DMA
    flops = 10 * n * rows * width * hidden
    return pl.pallas_call(
        functools.partial(step_kernel, n, loss_scale),
        out_shape=(
            jax.ShapeDtypeStruct((1, rows, width), F32),
            jax.ShapeDtypeStruct((wide, hidden), F32),
        ),
        in_specs=[
            pl.BlockSpec(memory_space=pltpu.SMEM), held, held,
            vmem, held, held, held,
            vmem, held, held, held,
        ],
        out_specs=(held, held),
        scratch_shapes=[
            pltpu.VMEM((1, rows, width), F32),
            pltpu.VMEM((wide, hidden), F32),
            pltpu.VMEM((1, hidden), F32),
            pltpu.VMEM((1, hidden), F32),
            pltpu.VMEM((width, hidden), BF),
            pltpu.VMEM((width, hidden), BF),
            pltpu.VMEM((hidden, width), BF),
            pltpu.VMEM((hidden, wide), BF),
            pltpu.VMEM((n, rows, width), BF),
            pltpu.VMEM((rows, width), BF),
            pltpu.VMEM((rows, hidden), BF),
            pltpu.VMEM((n, rows, width), BF),
            pltpu.VMEM((n + 1, rows, width), BF),
            pltpu.VMEM((n + 1, rows, width), BF),
            pltpu.VMEM((8, n * rows, hidden), BF),
            pltpu.VMEM((rows, width), BF),
            pltpu.VMEM((8, rows, wide), BF),
            pltpu.VMEM((8, rows, wide), BF),
            pltpu.VMEM((8, rows, wide), BF),
            pltpu.VMEM((rows, piece), F32),
            dma((7,)),
            dma((CHIPS,)),
            dma((2, n)),
            dma((n,)),
            dma((n, CHIPS)),
            dma((n + 1, CHIPS)),
            dma((n, CHIPS)),
            dma((n + 1, CHIPS)),
            dma((8,)),
            dma((8,)),
            dma((8, n)),
            dma((8, n)),
            dma((8,)),
            dma((8,)),
            dma((8,)),
            dma((8,)),
            dma((hidden // TILE + 1,)),
            dma((2, n, CHIPS)),
            dma((n, CHIPS)),
        ],
        compiler_params=pltpu.CompilerParams(
            collective_id=0, has_side_effects=True, vmem_limit_bytes=67043328
        ),
        cost_estimate=pl.CostEstimate(flops=flops, bytes_accessed=flops // 512, transcendentals=0),
    )(
        steps_t, x_gen, fresh_noise,
        real_mod, real_w_up, real_b_up, real_w_down,
        fake_mod, fake_w_up, fake_b_up, fake_w_down,
    )


def layer_norm(values):
    center = values - jnp.mean(values, axis=-1, keepdims=True)
    spread = jnp.mean(center * center, axis=-1, keepdims=True)
    return center * lax.rsqrt(spread + 1e-06)


def halves(block):
    cut = block.shape[0] // 2
    return [block[:cut], block[cut:]]


def add(a, b):
    return a.astype(F32) + b.astype(F32)


def ring_shift(value, step):
    n = lax.axis_size("gx")
    return lax.ppermute(value, "gx", [(i, (i + step) % n) for i in range(n)])


def flip(value, bit):
    n = lax.axis_size("gy")
    return lax.ppermute(value, "gy", [(i, i ^ bit) for i in range(n)])


def ring_gather(own):
    n = lax.axis_size("gx")
    blocks = {0: own}
    if n == 1:
        return blocks
    far = n // 2
    for d in range(1, far):
        blocks[n - d] = ring_shift(blocks[(n - d + 1) % n], 1)
        blocks[d] = ring_shift(blocks[d - 1], -1)
    first = ring_shift(halves(blocks[(n - far + 1) % n])[0], 1)
    second = ring_shift(halves(blocks[far - 1])[1], -1)
    blocks[far] = jnp.concatenate([first, second], axis=0)
    return blocks


def ring_scatter(parts):
    n = lax.axis_size("gx")
    cut = [halves(part) for part in parts]
    total = [half.astype(F32) for half in cut[0]]
    far = n // 2
    for half in (0, 1):
        for step in (1, -1):
            start = far if (half == 0) == (step == 1) else far - 1
            if start < 1:
                continue
            running = cut[(step * start) % n][half]
            for d in range(start, 0, -1):
                got = ring_shift(running, step)
                if d > 1:
                    running = add(cut[(step * (d - 1)) % n][half], got).astype(BF)
                else:
                    total[half] = total[half] + got.astype(F32)
    return jnp.concatenate(total, axis=0)


def route(k):
    return k & -k, 1 << (k.bit_length() - 1)


def chip_offsets(n):
    return sorted(range(2, n, 2), key=lambda k: (bin(k).count("1"), k))


def plane_gather(own):
    n = lax.axis_size("gy")
    blocks = {0: own}
    for k in chip_offsets(n):
        low, high = route(k)
        if low == high:
            blocks[k] = flip(own, k)
        else:
            first = flip(halves(blocks[k ^ low])[0], low)
            second = flip(halves(blocks[k ^ high])[1], high)
            blocks[k] = jnp.concatenate([first, second], axis=0)
    for k in range(0, n, 2):
        blocks[k + 1] = flip(blocks[k], 1)
    return blocks


def plane_scatter(parts):
    n = lax.axis_size("gy")
    held = {k: halves(add(parts[k], flip(parts[k + 1], 1))) for k in range(0, n, 2)}
    for k in reversed(chip_offsets(n)):
        low, high = route(k)
        for half, bit in ((0, low), (1, high)):
            got = flip(held[k][half].astype(BF), bit)
            held[k ^ bit][half] = held[k ^ bit][half] + got.astype(F32)
    return jnp.concatenate(held[0], axis=0)


def plain(
    x_gen,
    fresh_noise,
    steps_t,
    real_mod,
    real_w_up,
    real_b_up,
    real_w_down,
    fake_mod,
    fake_w_up,
    fake_b_up,
    fake_w_down,
):
    n_gx, n_gy = lax.axis_size("gx"), lax.axis_size("gy")
    me = lax.axis_index("gy")
    noise_level = (steps_t[0].astype(F32) + 1.0) / TSTEPS
    clean_f = x_gen[0].astype(F32)
    drawn_f = fresh_noise[0].astype(F32)
    noised = ((1.0 - noise_level) * clean_f + noise_level * drawn_f).astype(BF)
    target = (drawn_f - clean_f).astype(BF)
    own_rows, width = noised.shape
    wide = fake_w_up.shape[0]

    up_blocks = plane_gather(fake_w_up)
    tokens = ring_gather(noised)
    down_blocks = plane_gather(fake_w_down)

    def columns(array, k):
        return lax.dynamic_slice_in_dim(array, (me ^ k) * wide, wide, axis=1)

    noised_all = jnp.concatenate([tokens[j] for j in range(n_gx)], axis=0)
    normed = layer_norm(noised_all.astype(F32))
    real_in = (normed * (1.0 + real_mod[0, 1]) + real_mod[0, 0]).astype(BF)
    fake_in = (normed * (1.0 + fake_mod[0, 1]) + fake_mod[0, 0]).astype(BF)
    real_in, fake_in = lax.optimization_barrier((real_in, fake_in))
    real_hidden = jax.nn.gelu(
        jnp.dot(real_in, real_w_up, preferred_element_type=F32) + real_b_up, approximate=True
    ).astype(BF)
    real_part = jnp.dot(real_hidden, real_w_down, preferred_element_type=F32).astype(BF)
    real_rows = ring_scatter([real_part[j * own_rows:(j + 1) * own_rows] for j in range(n_gx)])

    fake_pre = fake_b_up[None]
    for k in range(n_gy):
        fake_pre = fake_pre + jnp.dot(
            columns(fake_in, k), up_blocks[k], preferred_element_type=F32
        )
    fake_hidden = jax.nn.gelu(fake_pre, approximate=True).astype(BF)

    loss_scale = float(n_gy * n_gx * own_rows) ** (-0.5)
    dmd_grad = jnp.zeros((own_rows, width), F32)
    products = {}
    for k in range(0, n_gy, 2):
        pair = jnp.concatenate(
            [
                jnp.dot(fake_hidden, down_blocks[i], preferred_element_type=F32).astype(BF)
                for i in (k, k + 1)
            ],
            axis=1,
        )
        pred = ring_scatter([pair[j * own_rows:(j + 1) * own_rows] for j in range(n_gx)])
        goal = jnp.concatenate([columns(target, i) for i in (k, k + 1)], axis=1)
        error = ring_gather((pred - goal.astype(F32)).astype(BF))
        error_all = jnp.concatenate([error[j] for j in range(n_gx)], axis=0)
        for i in (0, 1):
            part = slice(i * wide, (i + 1) * wide)
            dmd_grad = lax.dynamic_update_slice_in_dim(
                dmd_grad, pred[:, part], (me ^ (k + i)) * wide, axis=1
            )
            product = lax.dot_general(
                error_all[:, part],
                fake_hidden,
                (((0,), (0,)), ((), ())),
                preferred_element_type=F32,
            )
            products[k + i] = (product * loss_scale).astype(BF)
    fake_grad = plane_scatter(products)
    return ((dmd_grad - real_rows)[None], fake_grad)


def shards(*arrays):
    n_gx, n_gy = lax.axis_size("gx"), lax.axis_size("gy")
    width, hidden = arrays[4].shape
    wide = arrays[8].shape[0]
    fits = n_gy == 2 * CHIPS and n_gx >= 3 and wide % LANES == 0 and hidden % TILE == 0
    fits = fits and hidden >= width // 2 and width >= 2 * n_gx * arrays[0].shape[1]
    return one_kernel(*arrays) if fits else plain(*arrays)


def solution(mesh):
    return jax.shard_map(
        shards,
        mesh=mesh,
        in_specs=(
            P("gy", "gx", None),
            P("gy", "gx", None),
            P("gy"),
            P("gy", None, None),
            P(None, "gx"),
            P("gx"),
            P("gx", None),
            P("gy", None, None),
            P("gy", "gx"),
            P("gx"),
            P("gx", "gy"),
        ),
        out_specs=(P("gy", "gx", None), P("gy", "gx")),
        check_vma=False,
    )
```

```python
import functools

import jax
import jax.numpy as jnp
from jax import lax
from jax.experimental import pallas as pl
from jax.experimental.pallas import tpu as pltpu
from jax.sharding import PartitionSpec as P

TSTEPS = 1000
BF = jnp.bfloat16
F32 = jnp.float32
MESH = pl.DeviceIdType.MESH
LANES = 128
TILE = 256
CHIPS = 4


def widest(size):
    return max(s for s in (128, 256, 384, 512, 768) if size % s == 0)


def gelu(v):
    inner = 0.7978845608028654 * (v + 0.044715 * (v * v * v))
    return v * (0.5 * (1.0 + jnp.tanh(inner)))


def step_kernel(
    n,
    loss_scale,
    steps,
    x_hbm,
    noise_hbm,
    real_mod,
    real_up_hbm,
    real_bias_hbm,
    real_down_hbm,
    fake_mod,
    fake_up_hbm,
    fake_bias_hbm,
    fake_down_hbm,
    dmd_hbm,
    grad_hbm,
    dmd,
    grad,
    real_bias,
    fake_bias,
    up,
    real_up,
    real_down,
    fake_down,
    tokens,
    wide_in,
    real_hid,
    parts,
    recv,
    frecv,
    hid,
    target,
    goal,
    sent_pred,
    got_pred,
    total,
    local_sem,
    tile_sem,
    tok_send,
    tok_recv,
    rs_send,
    rs_recv,
    fs_send,
    fs_recv,
    up_send,
    up_recv,
    hid_send,
    hid_recv,
    goal_send,
    goal_recv,
    pred_send,
    pred_recv,
    out_sem,
    err_send,
    err_recv,
):
    z = lax.axis_index("gx")
    g = lax.axis_index("gy")
    rows, width = x_hbm.shape[1:]
    hidden = real_up_hbm.shape[1]
    wide = fake_up_hbm.shape[0]
    piece = width // CHIPS
    core = lax.rem(g, 2)
    bit_x = lax.rem(g // 2, 2)
    bit_y = lax.rem(g // 4, 2)

    def peer(k):
        other = g
        if k & 1:
            other = other + (1 - 2 * core)
        if k & 2:
            other = other + 2 * (1 - 2 * bit_x)
        if k & 4:
            other = other + 4 * (1 - 2 * bit_y)
        return other

    def remote(src, dst, send, got, to):
        return pltpu.make_async_remote_copy(
            src_ref=src, dst_ref=dst, send_sem=send, recv_sem=got,
            device_id=to, device_id_type=MESH,
        )

    def cols(k, size):
        start = k * size
        if not isinstance(k, int):
            start = pl.multiple_of(start, LANES)
        return pl.ds(start, size)

    def row_block(k, size):
        return pl.ds(pl.multiple_of(k * size, LANES), size)

    def arrived(ref, sem):
        remote(ref, ref, local_sem.at[0], sem, (z, peer(1))).wait_recv()

    def left(ref, sem):
        remote(ref, ref, sem, local_sem.at[0], (z, peer(1))).wait_send()

    not_first = z > 0
    not_last = z < n - 1
    between = not_first & not_last

    barrier = pltpu.get_barrier_semaphore()
    for k in range(1, 8):
        pl.semaphore_signal(barrier, inc=1, device_id=(z, peer(k)), device_id_type=MESH)

    @pl.when(not_first)
    def _():
        pl.semaphore_signal(barrier, inc=1, device_id=(z - 1, g), device_id_type=MESH)

    @pl.when(not_last)
    def _():
        pl.semaphore_signal(barrier, inc=1, device_id=(z + 1, g), device_id_type=MESH)

    load_x = pltpu.make_async_copy(x_hbm.at[0], parts.at[0], local_sem.at[0])
    load_noise = pltpu.make_async_copy(noise_hbm.at[0], parts.at[1], local_sem.at[1])
    load_own = pltpu.make_async_copy(fake_up_hbm, up.at[row_block(g, wide)], local_sem.at[2])
    load_real = pltpu.make_async_copy(real_up_hbm, real_up, local_sem.at[3])
    load_down = pltpu.make_async_copy(fake_down_hbm, fake_down, local_sem.at[4])
    load_real_bias = pltpu.make_async_copy(real_bias_hbm, real_bias.at[0], local_sem.at[5])
    load_fake_bias = pltpu.make_async_copy(fake_bias_hbm, fake_bias.at[0], local_sem.at[6])
    load_x.start()
    load_noise.start()
    load_real_bias.start()
    load_fake_bias.start()
    load_real.start()

    def load_tile(f):
        return pltpu.make_async_copy(
            real_down_hbm.at[:, cols(f, piece)], real_down.at[:, cols(f, piece)], tile_sem.at[f]
        )

    for f in range(CHIPS):
        load_tile(f).start()
    load_own.start()
    load_down.start()

    def token_copy(j, side):
        to = z + 1 if side == 0 else z - 1
        return remote(tokens.at[j], tokens.at[j], tok_send.at[side, j], tok_recv.at[j], (to, g))

    def up_copy(k, to):
        block = up.at[row_block(peer(k), wide)]
        source = fake_up_hbm if k == 0 else block
        return remote(source, block, up_send.at[k ^ to], up_recv.at[k ^ to], (z, peer(to)))

    def half_copy(array, send, got, row, size, k, to):
        half = size // 2
        block = array.at[pl.ds(pl.multiple_of(row + (0 if k == 2 else half), 32), half)]
        return remote(block, block, send.at[6 if k == 2 else 0], got.at[6], (z, peer(to)))

    def pass_up(k):
        up_wait(k)
        if k != 6:
            half_copy(up, up_send, up_recv, peer(k) * wide, wide, k, 6 - k).start()
        up_copy(k, 1).start()

    def goal_copy(k):
        return remote(
            target.at[:, cols(peer(k), wide)], goal.at[k], goal_send.at[k], goal_recv.at[k], (z, peer(k))
        )

    pl.semaphore_wait(barrier, 7 + jnp.minimum(z, 1) + jnp.minimum(n - 1 - z, 1))
    for to in (2, 4, 1):
        up_copy(0, to).start()

    load_x.wait()
    load_noise.wait()
    level = (jnp.full((1, LANES), steps[0].astype(F32), F32) + 1.0) / TSTEPS
    level = level[:, :1]

    def mix(i, carry):
        at = pl.ds(pl.multiple_of(i * 16, 16), 16)
        clean = parts[0, at, :].astype(F32)
        drawn = parts[1, at, :].astype(F32)
        tokens[z, at, :] = ((1.0 - level) * clean + level * drawn).astype(BF)
        target[at, :] = (drawn - clean).astype(BF)
        return carry

    quarter = rows // 4
    for part in range(4):
        lax.fori_loop(part * quarter // 16, (part + 1) * quarter // 16, mix, 0)
        block = tokens.at[z, pl.ds(part * quarter, quarter)]

        @pl.when(not_last)
        def _():
            remote(block, block, tok_send.at[0, z], tok_recv.at[z], (z + 1, g)).start()

        @pl.when(not_first)
        def _():
            remote(block, block, tok_send.at[1, z], tok_recv.at[z], (z - 1, g)).start()

    goal[0] = target[:, cols(g, wide)]

    def modulate(j, mod):
        def body(i, carry):
            at = pl.ds(pl.multiple_of(i * 16, 16), 16)
            v = tokens[j, at, :].astype(F32)
            center = v - jnp.mean(v, axis=-1, keepdims=True)
            spread = jnp.mean(center * center, axis=-1, keepdims=True)
            normed = center * lax.rsqrt(spread + 1e-06)
            wide_in[at, :] = (normed * (1.0 + mod[0, 1:2, :]) + mod[0, 0:1, :]).astype(BF)
            return carry

        lax.fori_loop(0, rows // 16, body, 0, unroll=4)

    def project(weights, bias, store):
        span = widest(hidden)

        def body(t, carry):
            at = cols(t, span)
            pre = jnp.dot(wide_in[...], weights[:, at], preferred_element_type=F32) + bias[:, at]
            store(at, gelu(pre).astype(BF))
            return carry

        lax.fori_loop(0, hidden // span, body, 0)

    both = jnp.minimum(z, n - 1 - z)

    def arrival(r):
        if r == 0:
            return z
        near = z - (r + 1) // 2 if r % 2 == 1 else z + r // 2
        far = jnp.where(z > n - 1 - z, z - (r - both), z + (r - both))
        return jnp.where(r <= 2 * both, near, far)

    def part_copy(buf, got, send, recv_sem, j, f, side):
        at = cols(f, piece)
        if side == 0:
            to, slot = z + 1, j + 1
        else:
            to, slot = z - 1, j
        return remote(
            buf.at[j, :, at], got.at[slot, :, at], send.at[j, f], recv_sem.at[slot, f], (to, g)
        )

    def pass_tokens(r):
        j = arrival(r)

        @pl.when(between)
        def _():
            arrived(tokens.at[j], tok_recv.at[j])

            @pl.when(j < z)
            def _():
                token_copy(j, 0).start()

            @pl.when(j > z)
            def _():
                token_copy(j, 1).start()

    def real_chunk(r):
        j = arrival(r)
        if r > 0:
            @pl.when(jnp.logical_not(between))
            def _():
                arrived(tokens.at[j], tok_recv.at[j])

        modulate(j, real_mod)
        if r == 0:
            load_real_bias.wait()
            load_real.wait()

        def keep(at, value):
            real_hid[:, at] = value

        project(real_up, real_bias, keep)
        for f in range(CHIPS):
            if r == 0:
                load_tile(f).wait()

            at = cols(f, piece)
            out = jnp.dot(real_hid[...], real_down[:, at], preferred_element_type=F32)
            parts[j, :, at] = out.astype(BF)
            if r > 0:
                @pl.when(z == 0)
                def _():
                    part_copy(parts, recv, rs_send, rs_recv, j, f, 0).start()

                @pl.when(z == n - 1)
                def _():
                    part_copy(parts, recv, rs_send, rs_recv, j, f, 1).start()

    def hid_copy(k, r, to):
        at = row_block(arrival(r), rows)
        return remote(
            hid.at[k, at], hid.at[k ^ to, at], hid_send.at[k ^ to, r], hid_recv.at[k ^ to, r],
            (z, peer(to)),
        )

    def fake_chunk(r):
        j = arrival(r)
        modulate(j, fake_mod)

        def keep(at, value):
            hid[0, row_block(j, rows), at] = value

        project(up, fake_bias, keep)
        for to in (2, 4, 1):
            hid_copy(0, r, to).start()

    def up_wait(k):
        arrived(up.at[row_block(peer(k), wide)], up_recv.at[k])

    def tokens_left():
        for j in range(n):
            @pl.when((j <= z) & not_last)
            def _():
                left(tokens.at[j], tok_send.at[0, j])

            @pl.when((j >= z) & not_first)
            def _():
                left(tokens.at[j], tok_send.at[1, j])

    def up_left():
        for k in range(8):
            parting = 2 if k in (0, 6) else 1
            left(fake_up_hbm.at[pl.ds(0, wide // parting)], up_send.at[k])

    def hid_wait(k):
        for r in range(n):
            start = pl.multiple_of(arrival(r) * rows, LANES)
            arrived(hid.at[k, pl.ds(start, rows)], hid_recv.at[k, r])
            if k in (2, 4):
                half = rows // 2
                at = pl.ds(pl.multiple_of(start + (0 if k == 2 else half), 16), half)
                remote(
                    hid.at[k, at], hid.at[6, at], hid_send.at[6 if k == 2 else 0, r], hid_recv.at[6, r],
                    (z, peer(6 - k)),
                ).start()
            if k in (2, 4, 6):
                hid_copy(k, r, 1).start()

    group = 2 if n % 2 == 0 else 1

    def fake_parts(c):
        for q in (0, 1):
            k = 2 * c + q

            def body(i, carry):
                out = jnp.dot(
                    hid[k, row_block(i, group * rows), :], fake_down[...], preferred_element_type=F32
                ).astype(BF)
                for s in range(group):
                    tokens[i * group + s, :, cols(k, wide)] = out[s * rows:(s + 1) * rows]
                return carry

            lax.fori_loop(0, n // group, body, 0)
        for e in range(n - 1, 0, -1):
            @pl.when(z == 0)
            def _():
                part_copy(tokens, frecv, fs_send, fs_recv, e, c, 0).start()

            @pl.when(z == n - 1)
            def _():
                part_copy(tokens, frecv, fs_send, fs_recv, n - 1 - e, c, 1).start()

    def part_wait(got, recv_sem, slot, f):
        arrived(got.at[slot, :, cols(f, piece)], recv_sem.at[slot, f])

    def relay(buf, got, send, recv_sem, f, right_owner, left_owner):
        at = cols(f, piece)
        for side, j in ((0, right_owner), (1, left_owner)):
            slot = j + 1 if side == 0 else j
            inside = (j > z) & (j < n) if side == 0 else (j >= 0) & (j < z)

            @pl.when(between & inside)
            def _():
                part_wait(got, recv_sem, slot, f)
                buf[j, :, at] = (buf[j, :, at].astype(F32) + got[slot, :, at].astype(F32)).astype(BF)
                part_copy(buf, got, send, recv_sem, j, f, side).start()

    def sum_own(buf, got, recv_sem, f):
        at = cols(f, piece)
        total[...] = buf[z, :, at].astype(F32)

        @pl.when(not_first)
        def _():
            part_wait(got, recv_sem, z + 1, f)
            total[...] += got[z + 1, :, at].astype(F32)

        @pl.when(not_last)
        def _():
            part_wait(got, recv_sem, z, f)
            total[...] += got[z, :, at].astype(F32)

    def relay_real(t, f):
        relay(parts, recv, rs_send, rs_recv, f, t - z, 2 * (n - 1) - t - z)

    def own_real():
        for f in range(CHIPS):
            sum_own(parts, recv, rs_recv, f)
            dmd[0, :, cols(f, piece)] = -total[...]

    def relay_fake(c, t):
        relay(tokens, frecv, fs_send, fs_recv, c, n - 1 + z - t, t - (n - 1 - z))

    def err_block(j, c):
        row = ((c // 2) * n + j) * rows
        return up.at[pl.ds(pl.multiple_of(row, LANES), rows), cols(c % 2, piece)]

    def err_copy(j, c, side):
        to = z + 1 if side == 0 else z - 1
        block = err_block(j, c)
        return remote(block, block, err_send.at[side, j, c], err_recv.at[j, c], (to, g))

    def pred_copy(k):
        return remote(
            sent_pred.at[k], got_pred.at[k], pred_send.at[k], pred_recv.at[k], (z, peer(k))
        )

    def own_fake(c):
        sum_own(tokens, frecv, fs_recv, c)
        for q in (0, 1):
            k = 2 * c + q
            if k > 0:
                arrived(goal.at[k], goal_recv.at[k])
            pred = total[:, q * wide:(q + 1) * wide]
            sent_pred[k] = pred.astype(BF)
            err_block(z, c)[:, q * wide:(q + 1) * wide] = (pred - goal[k].astype(F32)).astype(BF)

        @pl.when(not_last)
        def _():
            err_copy(z, c, 0).start()

        @pl.when(not_first)
        def _():
            err_copy(z, c, 1).start()

        for q in (0, 1):
            if 2 * c + q > 0:
                pred_copy(2 * c + q).start()

    def pass_side(c, d, side):
        j = z - d if side == 0 else z + d
        arrived(err_block(j, c), err_recv.at[j, c])
        err_copy(j, c, side).start()

    def pass_errors(c, d, inner):
        low = 2 * z < n

        @pl.when(between & (low if inner else jnp.logical_not(low)) & (z + d <= n - 1))
        def _():
            pass_side(c, d, 1)

        @pl.when(between & (jnp.logical_not(low) if inner else low) & (z - d >= 0))
        def _():
            pass_side(c, d, 0)

    def grad_out(t):
        return pltpu.make_async_copy(
            grad.at[:, cols(t, TILE)], grad_hbm.at[:, cols(t, TILE)], out_sem.at[t + 1]
        )

    def add_preds(c):
        for k in (2 * c, 2 * c + 1):
            if k > 0:
                arrived(got_pred.at[k], pred_recv.at[k])
            got = sent_pred[0] if k == 0 else got_pred[k]
            dmd[0, :, cols(peer(k), wide)] += got.astype(F32)

    def gradient(c):
        for j in range(n):
            @pl.when(jnp.logical_not(between) & (j != z))
            def _():
                arrived(err_block(j, c), err_recv.at[j, c])

        def body(t, carry):
            at = cols(t, TILE)
            out = jnp.zeros((wide, TILE), F32) if c == 0 else grad[:, at]
            for q in (0, 1):
                k = 2 * c + q
                row, col = (c // 2) * n * rows, (c % 2) * piece + q * wide
                errors = up[row:row + n * rows, col:col + wide]
                out = out + lax.dot_general(
                    errors, hid[k, :, at], (((0,), (0,)), ((), ())), preferred_element_type=F32
                )
            if c == CHIPS - 1:
                out = out * loss_scale
            grad[:, at] = out
            if c == CHIPS - 1:
                grad_out(t).start()
            return carry

        lax.fori_loop(0, hidden // TILE, body, 0)

    def later(c):
        for t in turns[1:]:
            relay_fake(c, t)

    def outer(c):
        pass_errors(c, 1, False)

    def far(c):
        for d in range(2, n - 1):
            pass_errors(c, d, True)
            pass_errors(c, d, False)

    hops = range(3, 2 * n - 2)
    turns = range(1, n - 1)
    real_chunk(0)
    for r in range(1, n - 1):
        if r % 2 == 1:
            for ahead in range(r, min(r + 2, n - 1)):
                pass_tokens(ahead)
        real_chunk(r)
        if r == 1:
            pass_up(2)
            pass_up(4)
            for k in range(1, 8):
                goal_copy(k).start()
    pass_tokens(n - 1)
    pass_up(6)
    load_own.wait()
    load_fake_bias.wait()
    load_down.wait()
    for k in (1, 3, 5, 7):
        up_wait(k)
    for r in range(n - 2):
        fake_chunk(r)
    for f in range(CHIPS - 1):
        relay_real(hops[0], f)
    real_chunk(n - 1)
    relay_real(hops[0], CHIPS - 1)
    fake_chunk(n - 2)
    for t in hops[1:-1]:
        for f in range(CHIPS // 2):
            relay_real(t, f)
    fake_chunk(n - 1)
    for t in hops[1:-1]:
        for f in range(CHIPS // 2, CHIPS):
            relay_real(t, f)
    tokens_left()
    up_left()
    hid_wait(1)
    fake_parts(0)
    for f in range(CHIPS):
        if len(hops) > 1:
            relay_real(hops[-1], f)
    relay_fake(0, 1)
    hid_wait(2)
    hid_wait(4)
    hid_wait(3)
    fake_parts(1)
    later(0)
    hid_wait(5)
    fake_parts(2)
    own_fake(0)
    relay_fake(1, 1)
    pass_errors(0, 1, True)
    later(1)
    hid_wait(6)
    hid_wait(7)
    fake_parts(3)
    own_fake(1)
    relay_fake(2, 1)
    pass_errors(1, 1, True)
    later(2)
    outer(0)
    own_fake(2)
    far(0)
    pass_errors(2, 1, True)
    relay_fake(3, 1)
    later(3)
    own_fake(3)
    outer(1)
    far(1)
    pass_errors(3, 1, True)
    outer(2)
    far(2)
    own_real()
    gradient(0)
    outer(3)
    gradient(1)
    far(3)
    for c in range(3):
        add_preds(c)
    gradient(2)
    add_preds(3)
    dmd_out = pltpu.make_async_copy(dmd, dmd_hbm, out_sem.at[0])
    dmd_out.start()
    gradient(3)

    for k in range(8):
        parting = 2 if k in (0, 6) else 1
        for r in range(n):
            left(hid.at[0, pl.ds(0, rows // parting)], hid_send.at[k, r])
    for k in range(1, 8):
        left(goal.at[k], goal_send.at[k])
        left(sent_pred.at[k], pred_send.at[k])
    for j in range(n):
        for f in range(CHIPS):
            @pl.when(j != z)
            def _():
                left(parts.at[j, :, cols(f, piece)], rs_send.at[j, f])
                left(tokens.at[j, :, cols(f, piece)], fs_send.at[j, f])

            @pl.when((j <= z) & not_last)
            def _():
                left(err_block(j, f), err_send.at[0, j, f])

            @pl.when((j >= z) & not_first)
            def _():
                left(err_block(j, f), err_send.at[1, j, f])
    for t in range(hidden // TILE):
        grad_out(t).wait()
    dmd_out.wait()


def one_kernel(
    x_gen, fresh_noise, steps_t, real_mod, real_w_up, real_b_up, real_w_down,
    fake_mod, fake_w_up, fake_b_up, fake_w_down,
):
    n = lax.axis_size("gx")
    rows, width = x_gen.shape[1:]
    hidden = real_w_up.shape[1]
    wide = fake_w_up.shape[0]
    piece = width // CHIPS
    loss_scale = float(lax.axis_size("gy") * n * rows) ** (-0.5)
    vmem = pl.BlockSpec(memory_space=pltpu.VMEM)
    held = pl.BlockSpec(memory_space=pl.ANY)
    dma = pltpu.SemaphoreType.DMA
    flops = 10 * n * rows * width * hidden
    return pl.pallas_call(
        functools.partial(step_kernel, n, loss_scale),
        out_shape=(
            jax.ShapeDtypeStruct((1, rows, width), F32),
            jax.ShapeDtypeStruct((wide, hidden), F32),
        ),
        in_specs=[
            pl.BlockSpec(memory_space=pltpu.SMEM), held, held,
            vmem, held, held, held,
            vmem, held, held, held,
        ],
        out_specs=(held, held),
        scratch_shapes=[
            pltpu.VMEM((1, rows, width), F32),
            pltpu.VMEM((wide, hidden), F32),
            pltpu.VMEM((1, hidden), F32),
            pltpu.VMEM((1, hidden), F32),
            pltpu.VMEM((width, hidden), BF),
            pltpu.VMEM((width, hidden), BF),
            pltpu.VMEM((hidden, width), BF),
            pltpu.VMEM((hidden, wide), BF),
            pltpu.VMEM((n, rows, width), BF),
            pltpu.VMEM((rows, width), BF),
            pltpu.VMEM((rows, hidden), BF),
            pltpu.VMEM((n, rows, width), BF),
            pltpu.VMEM((n + 1, rows, width), BF),
            pltpu.VMEM((n + 1, rows, width), BF),
            pltpu.VMEM((8, n * rows, hidden), BF),
            pltpu.VMEM((rows, width), BF),
            pltpu.VMEM((8, rows, wide), BF),
            pltpu.VMEM((8, rows, wide), BF),
            pltpu.VMEM((8, rows, wide), BF),
            pltpu.VMEM((rows, piece), F32),
            dma((7,)),
            dma((CHIPS,)),
            dma((2, n)),
            dma((n,)),
            dma((n, CHIPS)),
            dma((n + 1, CHIPS)),
            dma((n, CHIPS)),
            dma((n + 1, CHIPS)),
            dma((8,)),
            dma((8,)),
            dma((8, n)),
            dma((8, n)),
            dma((8,)),
            dma((8,)),
            dma((8,)),
            dma((8,)),
            dma((hidden // TILE + 1,)),
            dma((2, n, CHIPS)),
            dma((n, CHIPS)),
        ],
        compiler_params=pltpu.CompilerParams(
            collective_id=0, has_side_effects=True, vmem_limit_bytes=67043328
        ),
        cost_estimate=pl.CostEstimate(flops=flops, bytes_accessed=flops // 512, transcendentals=0),
    )(
        steps_t, x_gen, fresh_noise,
        real_mod, real_w_up, real_b_up, real_w_down,
        fake_mod, fake_w_up, fake_b_up, fake_w_down,
    )


def layer_norm(values):
    center = values - jnp.mean(values, axis=-1, keepdims=True)
    spread = jnp.mean(center * center, axis=-1, keepdims=True)
    return center * lax.rsqrt(spread + 1e-06)


def halves(block):
    cut = block.shape[0] // 2
    return [block[:cut], block[cut:]]


def add(a, b):
    return a.astype(F32) + b.astype(F32)


def ring_shift(value, step):
    n = lax.axis_size("gx")
    return lax.ppermute(value, "gx", [(i, (i + step) % n) for i in range(n)])


def flip(value, bit):
    n = lax.axis_size("gy")
    return lax.ppermute(value, "gy", [(i, i ^ bit) for i in range(n)])


def ring_gather(own):
    n = lax.axis_size("gx")
    blocks = {0: own}
    if n == 1:
        return blocks
    far = n // 2
    for d in range(1, far):
        blocks[n - d] = ring_shift(blocks[(n - d + 1) % n], 1)
        blocks[d] = ring_shift(blocks[d - 1], -1)
    first = ring_shift(halves(blocks[(n - far + 1) % n])[0], 1)
    second = ring_shift(halves(blocks[far - 1])[1], -1)
    blocks[far] = jnp.concatenate([first, second], axis=0)
    return blocks


def ring_scatter(parts):
    n = lax.axis_size("gx")
    cut = [halves(part) for part in parts]
    total = [half.astype(F32) for half in cut[0]]
    far = n // 2
    for half in (0, 1):
        for step in (1, -1):
            start = far if (half == 0) == (step == 1) else far - 1
            if start < 1:
                continue
            running = cut[(step * start) % n][half]
            for d in range(start, 0, -1):
                got = ring_shift(running, step)
                if d > 1:
                    running = add(cut[(step * (d - 1)) % n][half], got).astype(BF)
                else:
                    total[half] = total[half] + got.astype(F32)
    return jnp.concatenate(total, axis=0)


def route(k):
    return k & -k, 1 << (k.bit_length() - 1)


def chip_offsets(n):
    return sorted(range(2, n, 2), key=lambda k: (bin(k).count("1"), k))


def plane_gather(own):
    n = lax.axis_size("gy")
    blocks = {0: own}
    for k in chip_offsets(n):
        low, high = route(k)
        if low == high:
            blocks[k] = flip(own, k)
        else:
            first = flip(halves(blocks[k ^ low])[0], low)
            second = flip(halves(blocks[k ^ high])[1], high)
            blocks[k] = jnp.concatenate([first, second], axis=0)
    for k in range(0, n, 2):
        blocks[k + 1] = flip(blocks[k], 1)
    return blocks


def plane_scatter(parts):
    n = lax.axis_size("gy")
    held = {k: halves(add(parts[k], flip(parts[k + 1], 1))) for k in range(0, n, 2)}
    for k in reversed(chip_offsets(n)):
        low, high = route(k)
        for half, bit in ((0, low), (1, high)):
            got = flip(held[k][half].astype(BF), bit)
            held[k ^ bit][half] = held[k ^ bit][half] + got.astype(F32)
    return jnp.concatenate(held[0], axis=0)


def plain(
    x_gen,
    fresh_noise,
    steps_t,
    real_mod,
    real_w_up,
    real_b_up,
    real_w_down,
    fake_mod,
    fake_w_up,
    fake_b_up,
    fake_w_down,
):
    n_gx, n_gy = lax.axis_size("gx"), lax.axis_size("gy")
    me = lax.axis_index("gy")
    noise_level = (steps_t[0].astype(F32) + 1.0) / TSTEPS
    clean_f = x_gen[0].astype(F32)
    drawn_f = fresh_noise[0].astype(F32)
    noised = ((1.0 - noise_level) * clean_f + noise_level * drawn_f).astype(BF)
    target = (drawn_f - clean_f).astype(BF)
    own_rows, width = noised.shape
    wide = fake_w_up.shape[0]

    up_blocks = plane_gather(fake_w_up)
    tokens = ring_gather(noised)
    down_blocks = plane_gather(fake_w_down)

    def columns(array, k):
        return lax.dynamic_slice_in_dim(array, (me ^ k) * wide, wide, axis=1)

    noised_all = jnp.concatenate([tokens[j] for j in range(n_gx)], axis=0)
    normed = layer_norm(noised_all.astype(F32))
    real_in = (normed * (1.0 + real_mod[0, 1]) + real_mod[0, 0]).astype(BF)
    fake_in = (normed * (1.0 + fake_mod[0, 1]) + fake_mod[0, 0]).astype(BF)
    real_in, fake_in = lax.optimization_barrier((real_in, fake_in))
    real_hidden = jax.nn.gelu(
        jnp.dot(real_in, real_w_up, preferred_element_type=F32) + real_b_up, approximate=True
    ).astype(BF)
    real_part = jnp.dot(real_hidden, real_w_down, preferred_element_type=F32).astype(BF)
    real_rows = ring_scatter([real_part[j * own_rows:(j + 1) * own_rows] for j in range(n_gx)])

    fake_pre = fake_b_up[None]
    for k in range(n_gy):
        fake_pre = fake_pre + jnp.dot(
            columns(fake_in, k), up_blocks[k], preferred_element_type=F32
        )
    fake_hidden = jax.nn.gelu(fake_pre, approximate=True).astype(BF)

    loss_scale = float(n_gy * n_gx * own_rows) ** (-0.5)
    dmd_grad = jnp.zeros((own_rows, width), F32)
    products = {}
    for k in range(0, n_gy, 2):
        pair = jnp.concatenate(
            [
                jnp.dot(fake_hidden, down_blocks[i], preferred_element_type=F32).astype(BF)
                for i in (k, k + 1)
            ],
            axis=1,
        )
        pred = ring_scatter([pair[j * own_rows:(j + 1) * own_rows] for j in range(n_gx)])
        goal = jnp.concatenate([columns(target, i) for i in (k, k + 1)], axis=1)
        error = ring_gather((pred - goal.astype(F32)).astype(BF))
        error_all = jnp.concatenate([error[j] for j in range(n_gx)], axis=0)
        for i in (0, 1):
            part = slice(i * wide, (i + 1) * wide)
            dmd_grad = lax.dynamic_update_slice_in_dim(
                dmd_grad, pred[:, part], (me ^ (k + i)) * wide, axis=1
            )
            product = lax.dot_general(
                error_all[:, part],
                fake_hidden,
                (((0,), (0,)), ((), ())),
                preferred_element_type=F32,
            )
            products[k + i] = (product * loss_scale).astype(BF)
    fake_grad = plane_scatter(products)
    return ((dmd_grad - real_rows)[None], fake_grad)


def shards(*arrays):
    n_gx, n_gy = lax.axis_size("gx"), lax.axis_size("gy")
    width, hidden = arrays[4].shape
    wide = arrays[8].shape[0]
    fits = n_gy == 2 * CHIPS and n_gx >= 3 and wide % LANES == 0 and hidden % TILE == 0
    fits = fits and hidden >= width // 2 and width >= 2 * n_gx * arrays[0].shape[1]
    return one_kernel(*arrays) if fits else plain(*arrays)


def solution(mesh):
    return jax.shard_map(
        shards,
        mesh=mesh,
        in_specs=(
            P("gy", "gx", None),
            P("gy", "gx", None),
            P("gy"),
            P("gy", None, None),
            P(None, "gx"),
            P("gx"),
            P("gx", None),
            P("gy", None, None),
            P("gy", "gx"),
            P("gx"),
            P("gx", "gy"),
        ),
        out_specs=(P("gy", "gx", None), P("gy", "gx")),
        check_vma=False,
    )
```

```python
import functools

import jax
import jax.numpy as jnp
from jax import lax
from jax.experimental import pallas as pl
from jax.experimental.pallas import tpu as pltpu
from jax.sharding import PartitionSpec as P

TSTEPS = 1000
BF = jnp.bfloat16
F32 = jnp.float32
MESH = pl.DeviceIdType.MESH
LANES = 128
TILE = 256
CHIPS = 4


def widest(size):
    return max(s for s in (128, 256, 384, 512, 768) if size % s == 0)


def gelu(v):
    inner = 0.7978845608028654 * (v + 0.044715 * (v * v * v))
    return v * (0.5 * (1.0 + jnp.tanh(inner)))


def step_kernel(
    n,
    loss_scale,
    steps,
    x_hbm,
    noise_hbm,
    real_mod,
    real_up_hbm,
    real_bias_hbm,
    real_down_hbm,
    fake_mod,
    fake_up_hbm,
    fake_bias_hbm,
    fake_down_hbm,
    dmd_hbm,
    grad_hbm,
    dmd,
    grad,
    real_bias,
    fake_bias,
    up,
    real_up,
    real_down,
    fake_down,
    tokens,
    wide_in,
    real_hid,
    parts,
    recv,
    frecv,
    hid,
    target,
    goal,
    sent_pred,
    got_pred,
    total,
    local_sem,
    tile_sem,
    tok_send,
    tok_recv,
    rs_send,
    rs_recv,
    fs_send,
    fs_recv,
    up_send,
    up_recv,
    hid_send,
    hid_recv,
    goal_send,
    goal_recv,
    pred_send,
    pred_recv,
    out_sem,
    err_send,
    err_recv,
):
    z = lax.axis_index("gx")
    g = lax.axis_index("gy")
    rows, width = x_hbm.shape[1:]
    hidden = real_up_hbm.shape[1]
    wide = fake_up_hbm.shape[0]
    piece = width // CHIPS
    core = lax.rem(g, 2)
    bit_x = lax.rem(g // 2, 2)
    bit_y = lax.rem(g // 4, 2)

    def peer(k):
        other = g
        if k & 1:
            other = other + (1 - 2 * core)
        if k & 2:
            other = other + 2 * (1 - 2 * bit_x)
        if k & 4:
            other = other + 4 * (1 - 2 * bit_y)
        return other

    def remote(src, dst, send, got, to):
        return pltpu.make_async_remote_copy(
            src_ref=src, dst_ref=dst, send_sem=send, recv_sem=got,
            device_id=to, device_id_type=MESH,
        )

    def cols(k, size):
        start = k * size
        if not isinstance(k, int):
            start = pl.multiple_of(start, LANES)
        return pl.ds(start, size)

    def row_block(k, size):
        return pl.ds(pl.multiple_of(k * size, LANES), size)

    def arrived(ref, sem):
        remote(ref, ref, local_sem.at[0], sem, (z, peer(1))).wait_recv()

    def left(ref, sem):
        remote(ref, ref, sem, local_sem.at[0], (z, peer(1))).wait_send()

    not_first = z > 0
    not_last = z < n - 1
    between = not_first & not_last

    barrier = pltpu.get_barrier_semaphore()
    for k in range(1, 8):
        pl.semaphore_signal(barrier, inc=1, device_id=(z, peer(k)), device_id_type=MESH)

    @pl.when(not_first)
    def _():
        pl.semaphore_signal(barrier, inc=1, device_id=(z - 1, g), device_id_type=MESH)

    @pl.when(not_last)
    def _():
        pl.semaphore_signal(barrier, inc=1, device_id=(z + 1, g), device_id_type=MESH)

    load_x = pltpu.make_async_copy(x_hbm.at[0], parts.at[0], local_sem.at[0])
    load_noise = pltpu.make_async_copy(noise_hbm.at[0], parts.at[1], local_sem.at[1])
    load_own = pltpu.make_async_copy(fake_up_hbm, up.at[row_block(g, wide)], local_sem.at[2])
    load_real = pltpu.make_async_copy(real_up_hbm, real_up, local_sem.at[3])
    load_down = pltpu.make_async_copy(fake_down_hbm, fake_down, local_sem.at[4])
    load_real_bias = pltpu.make_async_copy(real_bias_hbm, real_bias.at[0], local_sem.at[5])
    load_fake_bias = pltpu.make_async_copy(fake_bias_hbm, fake_bias.at[0], local_sem.at[6])
    load_x.start()
    load_noise.start()
    load_real_bias.start()
    load_fake_bias.start()
    load_real.start()

    def load_tile(f):
        return pltpu.make_async_copy(
            real_down_hbm.at[:, cols(f, piece)], real_down.at[:, cols(f, piece)], tile_sem.at[f]
        )

    for f in range(CHIPS):
        load_tile(f).start()
    load_own.start()
    load_down.start()

    def token_copy(j, side):
        to = z + 1 if side == 0 else z - 1
        return remote(tokens.at[j], tokens.at[j], tok_send.at[side, j], tok_recv.at[j], (to, g))

    def up_copy(k, to):
        block = up.at[row_block(peer(k), wide)]
        source = fake_up_hbm if k == 0 else block
        return remote(source, block, up_send.at[k ^ to], up_recv.at[k ^ to], (z, peer(to)))

    def half_copy(array, send, got, row, size, k, to):
        half = size // 2
        block = array.at[pl.ds(pl.multiple_of(row + (0 if k == 2 else half), 32), half)]
        return remote(block, block, send.at[6 if k == 2 else 0], got.at[6], (z, peer(to)))

    def pass_up(k):
        up_wait(k)
        if k != 6:
            half_copy(up, up_send, up_recv, peer(k) * wide, wide, k, 6 - k).start()
        up_copy(k, 1).start()

    def goal_copy(k):
        return remote(
            target.at[:, cols(peer(k), wide)], goal.at[k], goal_send.at[k], goal_recv.at[k], (z, peer(k))
        )

    pl.semaphore_wait(barrier, 7 + jnp.minimum(z, 1) + jnp.minimum(n - 1 - z, 1))
    for to in (2, 4, 1):
        up_copy(0, to).start()

    load_x.wait()
    load_noise.wait()
    level = (jnp.full((1, LANES), steps[0].astype(F32), F32) + 1.0) / TSTEPS
    level = level[:, :1]

    def mix(i, carry):
        at = pl.ds(pl.multiple_of(i * 16, 16), 16)
        clean = parts[0, at, :].astype(F32)
        drawn = parts[1, at, :].astype(F32)
        tokens[z, at, :] = ((1.0 - level) * clean + level * drawn).astype(BF)
        target[at, :] = (drawn - clean).astype(BF)
        return carry

    quarter = rows // 4
    for part in range(4):
        lax.fori_loop(part * quarter // 16, (part + 1) * quarter // 16, mix, 0)
        block = tokens.at[z, pl.ds(part * quarter, quarter)]

        @pl.when(not_last)
        def _():
            remote(block, block, tok_send.at[0, z], tok_recv.at[z], (z + 1, g)).start()

        @pl.when(not_first)
        def _():
            remote(block, block, tok_send.at[1, z], tok_recv.at[z], (z - 1, g)).start()

    goal[0] = target[:, cols(g, wide)]

    def modulate(j, mod):
        def body(i, carry):
            at = pl.ds(pl.multiple_of(i * 16, 16), 16)
            v = tokens[j, at, :].astype(F32)
            center = v - jnp.mean(v, axis=-1, keepdims=True)
            spread = jnp.mean(center * center, axis=-1, keepdims=True)
            normed = center * lax.rsqrt(spread + 1e-06)
            wide_in[at, :] = (normed * (1.0 + mod[0, 1:2, :]) + mod[0, 0:1, :]).astype(BF)
            return carry

        lax.fori_loop(0, rows // 16, body, 0, unroll=4)

    def project(weights, bias, store):
        span = widest(hidden)

        def body(t, carry):
            at = cols(t, span)
            pre = jnp.dot(wide_in[...], weights[:, at], preferred_element_type=F32) + bias[:, at]
            store(at, gelu(pre).astype(BF))
            return carry

        lax.fori_loop(0, hidden // span, body, 0)

    both = jnp.minimum(z, n - 1 - z)

    def arrival(r):
        if r == 0:
            return z
        near = z - (r + 1) // 2 if r % 2 == 1 else z + r // 2
        far = jnp.where(z > n - 1 - z, z - (r - both), z + (r - both))
        return jnp.where(r <= 2 * both, near, far)

    def part_copy(buf, got, send, recv_sem, j, f, side):
        at = cols(f, piece)
        if side == 0:
            to, slot = z + 1, j + 1
        else:
            to, slot = z - 1, j
        return remote(
            buf.at[j, :, at], got.at[slot, :, at], send.at[j, f], recv_sem.at[slot, f], (to, g)
        )

    def pass_tokens(r):
        j = arrival(r)

        @pl.when(between)
        def _():
            arrived(tokens.at[j], tok_recv.at[j])

            @pl.when(j < z)
            def _():
                token_copy(j, 0).start()

            @pl.when(j > z)
            def _():
                token_copy(j, 1).start()

    def real_chunk(r):
        j = arrival(r)
        if r > 0:
            @pl.when(jnp.logical_not(between))
            def _():
                arrived(tokens.at[j], tok_recv.at[j])

        modulate(j, real_mod)
        if r == 0:
            load_real_bias.wait()
            load_real.wait()

        def keep(at, value):
            real_hid[:, at] = value

        project(real_up, real_bias, keep)
        for f in range(CHIPS):
            if r == 0:
                load_tile(f).wait()

            at = cols(f, piece)
            out = jnp.dot(real_hid[...], real_down[:, at], preferred_element_type=F32)
            parts[j, :, at] = out.astype(BF)
            if r > 0:
                @pl.when(z == 0)
                def _():
                    part_copy(parts, recv, rs_send, rs_recv, j, f, 0).start()

                @pl.when(z == n - 1)
                def _():
                    part_copy(parts, recv, rs_send, rs_recv, j, f, 1).start()

    def hid_copy(k, r, to):
        at = row_block(arrival(r), rows)
        return remote(
            hid.at[k, at], hid.at[k ^ to, at], hid_send.at[k ^ to, r], hid_recv.at[k ^ to, r],
            (z, peer(to)),
        )

    def fake_chunk(r):
        j = arrival(r)
        modulate(j, fake_mod)

        def keep(at, value):
            hid[0, row_block(j, rows), at] = value

        project(up, fake_bias, keep)
        for to in (2, 4, 1):
            hid_copy(0, r, to).start()

    def up_wait(k):
        arrived(up.at[row_block(peer(k), wide)], up_recv.at[k])

    def tokens_left():
        for j in range(n):
            @pl.when((j <= z) & not_last)
            def _():
                left(tokens.at[j], tok_send.at[0, j])

            @pl.when((j >= z) & not_first)
            def _():
                left(tokens.at[j], tok_send.at[1, j])

    def up_left():
        for k in range(8):
            parting = 2 if k in (0, 6) else 1
            left(fake_up_hbm.at[pl.ds(0, wide // parting)], up_send.at[k])

    def hid_wait(k):
        for r in range(n):
            start = pl.multiple_of(arrival(r) * rows, LANES)
            arrived(hid.at[k, pl.ds(start, rows)], hid_recv.at[k, r])
            if k in (2, 4):
                half = rows // 2
                at = pl.ds(pl.multiple_of(start + (0 if k == 2 else half), 16), half)
                remote(
                    hid.at[k, at], hid.at[6, at], hid_send.at[6 if k == 2 else 0, r], hid_recv.at[6, r],
                    (z, peer(6 - k)),
                ).start()
            if k in (2, 4, 6):
                hid_copy(k, r, 1).start()

    group = 2 if n % 2 == 0 else 1

    def fake_parts(c):
        for q in (0, 1):
            k = 2 * c + q

            def body(i, carry):
                out = jnp.dot(
                    hid[k, row_block(i, group * rows), :], fake_down[...], preferred_element_type=F32
                ).astype(BF)
                for s in range(group):
                    tokens[i * group + s, :, cols(k, wide)] = out[s * rows:(s + 1) * rows]
                return carry

            lax.fori_loop(0, n // group, body, 0)
        for e in range(n - 1, 0, -1):
            @pl.when(z == 0)
            def _():
                part_copy(tokens, frecv, fs_send, fs_recv, e, c, 0).start()

            @pl.when(z == n - 1)
            def _():
                part_copy(tokens, frecv, fs_send, fs_recv, n - 1 - e, c, 1).start()

    def part_wait(got, recv_sem, slot, f):
        arrived(got.at[slot, :, cols(f, piece)], recv_sem.at[slot, f])

    def relay(buf, got, send, recv_sem, f, right_owner, left_owner):
        at = cols(f, piece)
        for side, j in ((0, right_owner), (1, left_owner)):
            slot = j + 1 if side == 0 else j
            inside = (j > z) & (j < n) if side == 0 else (j >= 0) & (j < z)

            @pl.when(between & inside)
            def _():
                part_wait(got, recv_sem, slot, f)
                buf[j, :, at] = (buf[j, :, at].astype(F32) + got[slot, :, at].astype(F32)).astype(BF)
                part_copy(buf, got, send, recv_sem, j, f, side).start()

    def sum_own(buf, got, recv_sem, f):
        at = cols(f, piece)
        total[...] = buf[z, :, at].astype(F32)

        @pl.when(not_first)
        def _():
            part_wait(got, recv_sem, z + 1, f)
            total[...] += got[z + 1, :, at].astype(F32)

        @pl.when(not_last)
        def _():
            part_wait(got, recv_sem, z, f)
            total[...] += got[z, :, at].astype(F32)

    def relay_real(t, f):
        relay(parts, recv, rs_send, rs_recv, f, t - z, 2 * (n - 1) - t - z)

    def own_real():
        for f in range(CHIPS):
            sum_own(parts, recv, rs_recv, f)
            dmd[0, :, cols(f, piece)] = -total[...]

    def relay_fake(c, t):
        relay(tokens, frecv, fs_send, fs_recv, c, n - 1 + z - t, t - (n - 1 - z))

    def err_block(j, c):
        row = ((c // 2) * n + j) * rows
        return up.at[pl.ds(pl.multiple_of(row, LANES), rows), cols(c % 2, piece)]

    def err_copy(j, c, side):
        to = z + 1 if side == 0 else z - 1
        block = err_block(j, c)
        return remote(block, block, err_send.at[side, j, c], err_recv.at[j, c], (to, g))

    def pred_copy(k):
        return remote(
            sent_pred.at[k], got_pred.at[k], pred_send.at[k], pred_recv.at[k], (z, peer(k))
        )

    def own_fake(c):
        sum_own(tokens, frecv, fs_recv, c)
        for q in (0, 1):
            k = 2 * c + q
            if k > 0:
                arrived(goal.at[k], goal_recv.at[k])
            pred = total[:, q * wide:(q + 1) * wide]
            sent_pred[k] = pred.astype(BF)
            err_block(z, c)[:, q * wide:(q + 1) * wide] = (pred - goal[k].astype(F32)).astype(BF)

        @pl.when(not_last)
        def _():
            err_copy(z, c, 0).start()

        @pl.when(not_first)
        def _():
            err_copy(z, c, 1).start()

        for q in (0, 1):
            if 2 * c + q > 0:
                pred_copy(2 * c + q).start()

    def pass_side(c, d, side):
        j = z - d if side == 0 else z + d
        arrived(err_block(j, c), err_recv.at[j, c])
        err_copy(j, c, side).start()

    def pass_errors(c, d, inner):
        low = 2 * z < n

        @pl.when(between & (low if inner else jnp.logical_not(low)) & (z + d <= n - 1))
        def _():
            pass_side(c, d, 1)

        @pl.when(between & (jnp.logical_not(low) if inner else low) & (z - d >= 0))
        def _():
            pass_side(c, d, 0)

    step = 512 if hidden % 512 == 0 else TILE

    def grad_out(t):
        return pltpu.make_async_copy(
            grad.at[:, cols(t, step)], grad_hbm.at[:, cols(t, step)], out_sem.at[t + 1]
        )

    def add_preds(c):
        for k in (2 * c, 2 * c + 1):
            if k > 0:
                arrived(got_pred.at[k], pred_recv.at[k])
            got = sent_pred[0] if k == 0 else got_pred[k]
            dmd[0, :, cols(peer(k), wide)] += got.astype(F32)

    def gradient(c):
        for j in range(n):
            @pl.when(jnp.logical_not(between) & (j != z))
            def _():
                arrived(err_block(j, c), err_recv.at[j, c])

        def body(t, carry):
            at = cols(t, step)
            out = jnp.zeros((wide, step), F32) if c == 0 else grad[:, at]
            for q in (0, 1):
                k = 2 * c + q
                row, col = (c // 2) * n * rows, (c % 2) * piece + q * wide
                errors = up[row:row + n * rows, col:col + wide]
                out = out + lax.dot_general(
                    errors, hid[k, :, at], (((0,), (0,)), ((), ())), preferred_element_type=F32
                )
            if c == CHIPS - 1:
                out = out * loss_scale
            grad[:, at] = out
            if c == CHIPS - 1:
                grad_out(t).start()
            return carry

        lax.fori_loop(0, hidden // step, body, 0)

    def later(c):
        for t in turns[1:]:
            relay_fake(c, t)

    def outer(c):
        pass_errors(c, 1, False)

    def far(c):
        for d in range(2, n - 1):
            pass_errors(c, d, True)
            pass_errors(c, d, False)

    hops = range(3, 2 * n - 2)
    turns = range(1, n - 1)
    real_chunk(0)
    for r in range(1, n - 1):
        if r % 2 == 1:
            for ahead in range(r, min(r + 2, n - 1)):
                pass_tokens(ahead)
        real_chunk(r)
        if r == 1:
            pass_up(2)
            pass_up(4)
            for k in range(1, 8):
                goal_copy(k).start()
    pass_tokens(n - 1)
    pass_up(6)
    load_own.wait()
    load_fake_bias.wait()
    load_down.wait()
    for k in (1, 3, 5, 7):
        up_wait(k)
    for r in range(n - 2):
        fake_chunk(r)
    for f in range(CHIPS - 1):
        relay_real(hops[0], f)
    real_chunk(n - 1)
    relay_real(hops[0], CHIPS - 1)
    fake_chunk(n - 2)
    for t in hops[1:-1]:
        for f in range(CHIPS // 2):
            relay_real(t, f)
    fake_chunk(n - 1)
    for t in hops[1:-1]:
        for f in range(CHIPS // 2, CHIPS):
            relay_real(t, f)
    tokens_left()
    up_left()
    hid_wait(1)
    fake_parts(0)
    for f in range(CHIPS):
        if len(hops) > 1:
            relay_real(hops[-1], f)
    relay_fake(0, 1)
    hid_wait(2)
    hid_wait(4)
    hid_wait(3)
    fake_parts(1)
    later(0)
    hid_wait(5)
    fake_parts(2)
    own_fake(0)
    relay_fake(1, 1)
    pass_errors(0, 1, True)
    later(1)
    relay_fake(2, 1)
    hid_wait(6)
    hid_wait(7)
    fake_parts(3)
    own_fake(1)
    later(2)
    pass_errors(1, 1, True)
    relay_fake(3, 1)
    own_fake(2)
    later(3)
    outer(0)
    pass_errors(2, 1, True)
    outer(1)
    own_fake(3)
    far(0)
    far(1)
    pass_errors(3, 1, True)
    outer(2)
    far(2)
    own_real()
    gradient(0)
    outer(3)
    gradient(1)
    far(3)
    for c in range(3):
        add_preds(c)
    gradient(2)
    add_preds(3)
    dmd_out = pltpu.make_async_copy(dmd, dmd_hbm, out_sem.at[0])
    dmd_out.start()
    gradient(3)

    for k in range(8):
        parting = 2 if k in (0, 6) else 1
        for r in range(n):
            left(hid.at[0, pl.ds(0, rows // parting)], hid_send.at[k, r])
    for k in range(1, 8):
        left(goal.at[k], goal_send.at[k])
        left(sent_pred.at[k], pred_send.at[k])
    for j in range(n):
        for f in range(CHIPS):
            @pl.when(j != z)
            def _():
                left(parts.at[j, :, cols(f, piece)], rs_send.at[j, f])
                left(tokens.at[j, :, cols(f, piece)], fs_send.at[j, f])

            @pl.when((j <= z) & not_last)
            def _():
                left(err_block(j, f), err_send.at[0, j, f])

            @pl.when((j >= z) & not_first)
            def _():
                left(err_block(j, f), err_send.at[1, j, f])
    for t in range(hidden // step):
        grad_out(t).wait()
    dmd_out.wait()


def one_kernel(
    x_gen, fresh_noise, steps_t, real_mod, real_w_up, real_b_up, real_w_down,
    fake_mod, fake_w_up, fake_b_up, fake_w_down,
):
    n = lax.axis_size("gx")
    rows, width = x_gen.shape[1:]
    hidden = real_w_up.shape[1]
    wide = fake_w_up.shape[0]
    piece = width // CHIPS
    loss_scale = float(lax.axis_size("gy") * n * rows) ** (-0.5)
    vmem = pl.BlockSpec(memory_space=pltpu.VMEM)
    held = pl.BlockSpec(memory_space=pl.ANY)
    dma = pltpu.SemaphoreType.DMA
    flops = 10 * n * rows * width * hidden
    return pl.pallas_call(
        functools.partial(step_kernel, n, loss_scale),
        out_shape=(
            jax.ShapeDtypeStruct((1, rows, width), F32),
            jax.ShapeDtypeStruct((wide, hidden), F32),
        ),
        in_specs=[
            pl.BlockSpec(memory_space=pltpu.SMEM), held, held,
            vmem, held, held, held,
            vmem, held, held, held,
        ],
        out_specs=(held, held),
        scratch_shapes=[
            pltpu.VMEM((1, rows, width), F32),
            pltpu.VMEM((wide, hidden), F32),
            pltpu.VMEM((1, hidden), F32),
            pltpu.VMEM((1, hidden), F32),
            pltpu.VMEM((width, hidden), BF),
            pltpu.VMEM((width, hidden), BF),
            pltpu.VMEM((hidden, width), BF),
            pltpu.VMEM((hidden, wide), BF),
            pltpu.VMEM((n, rows, width), BF),
            pltpu.VMEM((rows, width), BF),
            pltpu.VMEM((rows, hidden), BF),
            pltpu.VMEM((n, rows, width), BF),
            pltpu.VMEM((n + 1, rows, width), BF),
            pltpu.VMEM((n + 1, rows, width), BF),
            pltpu.VMEM((8, n * rows, hidden), BF),
            pltpu.VMEM((rows, width), BF),
            pltpu.VMEM((8, rows, wide), BF),
            pltpu.VMEM((8, rows, wide), BF),
            pltpu.VMEM((8, rows, wide), BF),
            pltpu.VMEM((rows, piece), F32),
            dma((7,)),
            dma((CHIPS,)),
            dma((2, n)),
            dma((n,)),
            dma((n, CHIPS)),
            dma((n + 1, CHIPS)),
            dma((n, CHIPS)),
            dma((n + 1, CHIPS)),
            dma((8,)),
            dma((8,)),
            dma((8, n)),
            dma((8, n)),
            dma((8,)),
            dma((8,)),
            dma((8,)),
            dma((8,)),
            dma((hidden // TILE + 1,)),
            dma((2, n, CHIPS)),
            dma((n, CHIPS)),
        ],
        compiler_params=pltpu.CompilerParams(
            collective_id=0, has_side_effects=True, vmem_limit_bytes=67043328
        ),
        cost_estimate=pl.CostEstimate(flops=flops, bytes_accessed=flops // 512, transcendentals=0),
    )(
        steps_t, x_gen, fresh_noise,
        real_mod, real_w_up, real_b_up, real_w_down,
        fake_mod, fake_w_up, fake_b_up, fake_w_down,
    )


def layer_norm(values):
    center = values - jnp.mean(values, axis=-1, keepdims=True)
    spread = jnp.mean(center * center, axis=-1, keepdims=True)
    return center * lax.rsqrt(spread + 1e-06)


def halves(block):
    cut = block.shape[0] // 2
    return [block[:cut], block[cut:]]


def add(a, b):
    return a.astype(F32) + b.astype(F32)


def ring_shift(value, step):
    n = lax.axis_size("gx")
    return lax.ppermute(value, "gx", [(i, (i + step) % n) for i in range(n)])


def flip(value, bit):
    n = lax.axis_size("gy")
    return lax.ppermute(value, "gy", [(i, i ^ bit) for i in range(n)])


def ring_gather(own):
    n = lax.axis_size("gx")
    blocks = {0: own}
    if n == 1:
        return blocks
    far = n // 2
    for d in range(1, far):
        blocks[n - d] = ring_shift(blocks[(n - d + 1) % n], 1)
        blocks[d] = ring_shift(blocks[d - 1], -1)
    first = ring_shift(halves(blocks[(n - far + 1) % n])[0], 1)
    second = ring_shift(halves(blocks[far - 1])[1], -1)
    blocks[far] = jnp.concatenate([first, second], axis=0)
    return blocks


def ring_scatter(parts):
    n = lax.axis_size("gx")
    cut = [halves(part) for part in parts]
    total = [half.astype(F32) for half in cut[0]]
    far = n // 2
    for half in (0, 1):
        for step in (1, -1):
            start = far if (half == 0) == (step == 1) else far - 1
            if start < 1:
                continue
            running = cut[(step * start) % n][half]
            for d in range(start, 0, -1):
                got = ring_shift(running, step)
                if d > 1:
                    running = add(cut[(step * (d - 1)) % n][half], got).astype(BF)
                else:
                    total[half] = total[half] + got.astype(F32)
    return jnp.concatenate(total, axis=0)


def route(k):
    return k & -k, 1 << (k.bit_length() - 1)


def chip_offsets(n):
    return sorted(range(2, n, 2), key=lambda k: (bin(k).count("1"), k))


def plane_gather(own):
    n = lax.axis_size("gy")
    blocks = {0: own}
    for k in chip_offsets(n):
        low, high = route(k)
        if low == high:
            blocks[k] = flip(own, k)
        else:
            first = flip(halves(blocks[k ^ low])[0], low)
            second = flip(halves(blocks[k ^ high])[1], high)
            blocks[k] = jnp.concatenate([first, second], axis=0)
    for k in range(0, n, 2):
        blocks[k + 1] = flip(blocks[k], 1)
    return blocks


def plane_scatter(parts):
    n = lax.axis_size("gy")
    held = {k: halves(add(parts[k], flip(parts[k + 1], 1))) for k in range(0, n, 2)}
    for k in reversed(chip_offsets(n)):
        low, high = route(k)
        for half, bit in ((0, low), (1, high)):
            got = flip(held[k][half].astype(BF), bit)
            held[k ^ bit][half] = held[k ^ bit][half] + got.astype(F32)
    return jnp.concatenate(held[0], axis=0)


def plain(
    x_gen,
    fresh_noise,
    steps_t,
    real_mod,
    real_w_up,
    real_b_up,
    real_w_down,
    fake_mod,
    fake_w_up,
    fake_b_up,
    fake_w_down,
):
    n_gx, n_gy = lax.axis_size("gx"), lax.axis_size("gy")
    me = lax.axis_index("gy")
    noise_level = (steps_t[0].astype(F32) + 1.0) / TSTEPS
    clean_f = x_gen[0].astype(F32)
    drawn_f = fresh_noise[0].astype(F32)
    noised = ((1.0 - noise_level) * clean_f + noise_level * drawn_f).astype(BF)
    target = (drawn_f - clean_f).astype(BF)
    own_rows, width = noised.shape
    wide = fake_w_up.shape[0]

    up_blocks = plane_gather(fake_w_up)
    tokens = ring_gather(noised)
    down_blocks = plane_gather(fake_w_down)

    def columns(array, k):
        return lax.dynamic_slice_in_dim(array, (me ^ k) * wide, wide, axis=1)

    noised_all = jnp.concatenate([tokens[j] for j in range(n_gx)], axis=0)
    normed = layer_norm(noised_all.astype(F32))
    real_in = (normed * (1.0 + real_mod[0, 1]) + real_mod[0, 0]).astype(BF)
    fake_in = (normed * (1.0 + fake_mod[0, 1]) + fake_mod[0, 0]).astype(BF)
    real_in, fake_in = lax.optimization_barrier((real_in, fake_in))
    real_hidden = jax.nn.gelu(
        jnp.dot(real_in, real_w_up, preferred_element_type=F32) + real_b_up, approximate=True
    ).astype(BF)
    real_part = jnp.dot(real_hidden, real_w_down, preferred_element_type=F32).astype(BF)
    real_rows = ring_scatter([real_part[j * own_rows:(j + 1) * own_rows] for j in range(n_gx)])

    fake_pre = fake_b_up[None]
    for k in range(n_gy):
        fake_pre = fake_pre + jnp.dot(
            columns(fake_in, k), up_blocks[k], preferred_element_type=F32
        )
    fake_hidden = jax.nn.gelu(fake_pre, approximate=True).astype(BF)

    loss_scale = float(n_gy * n_gx * own_rows) ** (-0.5)
    dmd_grad = jnp.zeros((own_rows, width), F32)
    products = {}
    for k in range(0, n_gy, 2):
        pair = jnp.concatenate(
            [
                jnp.dot(fake_hidden, down_blocks[i], preferred_element_type=F32).astype(BF)
                for i in (k, k + 1)
            ],
            axis=1,
        )
        pred = ring_scatter([pair[j * own_rows:(j + 1) * own_rows] for j in range(n_gx)])
        goal = jnp.concatenate([columns(target, i) for i in (k, k + 1)], axis=1)
        error = ring_gather((pred - goal.astype(F32)).astype(BF))
        error_all = jnp.concatenate([error[j] for j in range(n_gx)], axis=0)
        for i in (0, 1):
            part = slice(i * wide, (i + 1) * wide)
            dmd_grad = lax.dynamic_update_slice_in_dim(
                dmd_grad, pred[:, part], (me ^ (k + i)) * wide, axis=1
            )
            product = lax.dot_general(
                error_all[:, part],
                fake_hidden,
                (((0,), (0,)), ((), ())),
                preferred_element_type=F32,
            )
            products[k + i] = (product * loss_scale).astype(BF)
    fake_grad = plane_scatter(products)
    return ((dmd_grad - real_rows)[None], fake_grad)


def shards(*arrays):
    n_gx, n_gy = lax.axis_size("gx"), lax.axis_size("gy")
    width, hidden = arrays[4].shape
    wide = arrays[8].shape[0]
    fits = n_gy == 2 * CHIPS and n_gx >= 3 and wide % LANES == 0 and hidden % TILE == 0
    fits = fits and hidden >= width // 2 and width >= 2 * n_gx * arrays[0].shape[1]
    return one_kernel(*arrays) if fits else plain(*arrays)


def solution(mesh):
    return jax.shard_map(
        shards,
        mesh=mesh,
        in_specs=(
            P("gy", "gx", None),
            P("gy", "gx", None),
            P("gy"),
            P("gy", None, None),
            P(None, "gx"),
            P("gx"),
            P("gx", None),
            P("gy", None, None),
            P("gy", "gx"),
            P("gx"),
            P("gx", "gy"),
        ),
        out_specs=(P("gy", "gx", None), P("gy", "gx")),
        check_vma=False,
    )
```
